32 devices in a mesh: groups: 2 (over y), seq: 4 (over z), head: 2 (over x), inner: 2 (over core).
Axes of the slice: x: 2, y: 2, z: 4, core: 2. Of those that a mesh axis runs over, the one named last changes fastest.
Arguments:
- queries: bfloat16 [4096, 2, 8, 128], P(('groups', 'seq'), 'head', 'inner'), parts along dimension 0, may hold values from -120 to 120
- grad_out: bfloat16 [4096, 2, 8, 128], P(('groups', 'seq'), 'head', 'inner'), parts along dimension 0, may hold values from -6 to 6
- keys: bfloat16 [4096, 2, 128], P(('groups', 'seq'), 'head'), parts along dimension 0, may hold values from -6 to 6
- values: bfloat16 [4096, 2, 128], P(('groups', 'seq'), 'head'), parts along dimension 0, may hold values from -6 to 6
- indices: int32 [2, 64, 16], P('head', 'groups'), parts along dimension 1, may hold values from 0 to 31, as said below
- valid: int32 [2, 64, 16], P('head', 'groups'), parts along dimension 1, may hold values from 0 to 1
Outputs:
- grad_queries: bfloat16 [4096, 2, 8, 128], P(('groups', 'seq'), 'head', 'inner'), parts along dimension 0
- grad_keys: bfloat16 [4096, 2, 128], P(('groups', 'seq'), 'head'), parts along dimension 0
- grad_values: bfloat16 [4096, 2, 128], P(('groups', 'seq'), 'head'), parts along dimension 0
The draws below stay inside these ranges and needn't reach their ends.
There are 2 independent parts, one for each index of `groups`. The reference program is written for one: setup_inputs(seed, part) draws one part's arguments, and reference() takes and returns one part's arrays. A program takes and returns all parts, laid end to end along the dimension named above; each array names one. Nothing has to cross between parts.
Inputs may be any that keep to these rules, and one draw needn't show every extreme that they name: `indices`: call blocks r * 8 to r * 8 + 7 run r. For every KV head and query block b: slot 0 names b and is valid; the valid slots name distinct blocks at most b; over all query blocks of run r, the valid slots name blocks of runs later than r never, and for each earlier run exactly 4 distinct blocks of it. Slots that are not valid name arbitrary blocks.
All inputs are finite; a program needn't handle non-finite values.
Results may differ from the reference program's by a relative error of at most 0.007.
Values may be sent and summed in bfloat16 or wider, within the bound.
A program may use at most 64 MiB of HBM per device.

```python
import jax
import jax.numpy as jnp
from jax import lax

HD = 128
GQ = 8
KVH = 2
BLK = 64
TOPK = 16
CAP = 4
QBD = 8
NQB = 32
SEQ_LEN = 2048


def paired_fields(key):
    base = jax.random.fold_in(key, 11)
    query_key, other_key = jax.random.split(base)
    drawn_q = jnp.clip(jax.random.normal(query_key, (SEQ_LEN, KVH, GQ, HD), jnp.float32), -6.0, 6.0)
    drawn_k = jnp.clip(jax.random.normal(other_key, (SEQ_LEN, KVH, HD), jnp.float32), -6.0, 6.0)
    keys_out = drawn_k
    queries_out = drawn_q
    return (queries_out, keys_out)


def draw_queries(key, part):
    return paired_fields(key)[0].astype(jnp.bfloat16)


def draw_keys(key, part):
    return paired_fields(key)[1].astype(jnp.bfloat16)


def selection(key):
    base = jax.random.fold_in(key, 29)
    pool_key, noise_key, count_key = jax.random.split(base, 3)
    runs = NQB // QBD
    blocks = jnp.arange(NQB, dtype=jnp.int32)
    owner = blocks // QBD
    local = blocks % QBD
    pool_score = jax.random.randint(pool_key, (KVH, runs, runs, QBD), 0, 2 ** 20, jnp.int32) * QBD + jnp.arange(QBD, dtype=jnp.int32)
    order = jnp.argsort(-pool_score, axis=-1, stable=True)
    ranking = jnp.argsort(order, axis=-1, stable=True).astype(jnp.int32)
    in_pool = ranking < CAP
    pool_pair = in_pool[:, owner[:, None], owner[None, :], local[None, :]]
    pool_rank = ranking[:, owner[:, None], owner[None, :], local[None, :]]
    remote_ok = (owner[None, :] < owner[:, None])[None] & pool_pair
    own_ok = ((owner[None, :] == owner[:, None]) & (blocks[None, :] < blocks[:, None]))[None]
    is_self = (blocks[None, :] == blocks[:, None])[None]
    query_local = (blocks % QBD)[:, None][None]
    forced = remote_ok & ((owner[None, :] * CAP + pool_rank) % QBD == query_local)
    noise = jax.random.randint(noise_key, (KVH, NQB, NQB), 0, 2 ** 16, jnp.int32) * NQB + blocks
    score = noise + forced.astype(jnp.int32) * 2 ** 29 + is_self.astype(jnp.int32) * 2 ** 30
    score = jnp.where(is_self | own_ok | remote_ok, score, -1 - blocks)
    top_values, top_blocks = lax.top_k(score, TOPK)
    forced_count = jnp.sum(forced.astype(jnp.int32), axis=-1)
    drawn_count = jax.random.randint(count_key, (KVH, NQB), TOPK // 2, TOPK + 1, jnp.int32)
    keeping = jnp.maximum(drawn_count, 1 + forced_count)
    usable = (top_values >= 0) & (jnp.arange(TOPK, dtype=jnp.int32)[None, None, :] < keeping[..., None])
    return (top_blocks.astype(jnp.int32), usable.astype(jnp.int32))


def draw_indices(key, part):
    return selection(key)[0]


def draw_valid(key, part):
    return selection(key)[1]


def block_levels(rng, extent, cuts, low, high):
    loudness = 1.0
    for axis_at, blocks in cuts:
        draws = jax.random.uniform(jax.random.fold_in(jax.random.fold_in(rng, 6), axis_at), (blocks,), jnp.float32, low / len(cuts), high / len(cuts))
        loudness = loudness * jnp.repeat(jnp.exp(draws), extent[axis_at] // blocks).reshape((-1,) + (1,) * (len(extent) - 1 - axis_at))
    return loudness


def bell_draw(own_key, dims, deviation, limit, shards=(), kind=jnp.bfloat16):
    array = jax.random.normal(own_key, dims, jnp.float32) * deviation
    if len(shards) > 0:
        array = block_levels(own_key, dims, shards, -0.22, 0.18) * array
    return jnp.clip(array, min=-limit, max=limit).astype(kind)


def setup_inputs(seed: int = 0, part: int = 0) -> dict:
    arg_keys = jax.random.split(jax.random.key(seed), 7)
    part_splits = jax.random.split(jax.random.fold_in(arg_keys[6], part), 7)
    queries = draw_queries(jax.random.fold_in(jax.random.fold_in(arg_keys[6], part), 71), part)
    grad_out = bell_draw(part_splits[1], (SEQ_LEN, KVH, GQ, HD), 1.0, 6.0, ((0, 4), (1, 2), (2, 2)))
    keys = draw_keys(jax.random.fold_in(jax.random.fold_in(arg_keys[6], part), 71), part)
    values = bell_draw(part_splits[3], (SEQ_LEN, KVH, HD), 1.0, 6.0, ((0, 4), (1, 2)))
    indices = draw_indices(jax.random.fold_in(jax.random.fold_in(arg_keys[6], part), 71), part)
    valid = draw_valid(jax.random.fold_in(jax.random.fold_in(arg_keys[6], part), 71), part)
    return {"queries": queries, "grad_out": grad_out, "keys": keys, "values": values, "indices": indices, "valid": valid}


def reference(queries, grad_out, keys, values, indices, valid):
    scaling = 1.0 / jnp.sqrt(jnp.float32(HD))
    position = jnp.arange(BLK, dtype=jnp.int32)
    causal = position[None, :] <= position[:, None]

    def per_head(head):
        q_head = queries[:, head].reshape(NQB, BLK, GQ, HD)
        do_head = grad_out[:, head].reshape(NQB, BLK, GQ, HD)
        k_head = keys[:, head].reshape(NQB, BLK, HD)
        v_head = values[:, head].reshape(NQB, BLK, HD)

        def step(carry, inputs):
            key_acc, value_acc = carry
            q_block, do_block, picks, usable, block = inputs
            k_sel = k_head[picks].reshape(TOPK * BLK, HD).astype(jnp.float32)
            v_sel = v_head[picks].reshape(TOPK * BLK, HD).astype(jnp.float32)
            before = picks < block
            same = picks == block
            allowed = usable[None, :, None] & (before[None, :, None] | same[None, :, None] & causal[:, None, :])
            allowed = allowed.reshape(BLK, TOPK * BLK)[None]
            q_float = q_block.astype(jnp.float32)
            do_float = do_block.astype(jnp.float32)
            scores = jnp.einsum('igw,sw->gis', q_float, k_sel) * scaling
            highest = lax.optimization_barrier(jnp.max(jnp.where(allowed, scores, -jnp.inf), axis=-1, keepdims=True))
            weights = jnp.where(allowed, jnp.exp(scores - highest), 0.0)
            probs = weights / lax.optimization_barrier(jnp.sum(weights, axis=-1, keepdims=True))
            probs_b = probs.astype(jnp.bfloat16)
            dprobs = jnp.einsum('igw,sw->gis', do_float, v_sel)
            delta = lax.optimization_barrier(jnp.sum(probs * dprobs, axis=-1, keepdims=True))
            dscores = (probs * (dprobs - delta)).astype(jnp.bfloat16).astype(jnp.float32)
            grad_q = (jnp.einsum('gis,sw->igw', dscores, k_sel) * scaling).astype(jnp.bfloat16)
            key_terms = jnp.einsum('gis,igw->sw', dscores, q_float) * scaling
            value_terms = jnp.einsum('gis,igw->sw', probs_b.astype(jnp.float32), do_float)
            key_acc = key_acc.at[picks].add(key_terms.reshape(TOPK, BLK, HD))
            value_acc = value_acc.at[picks].add(value_terms.reshape(TOPK, BLK, HD))
            return ((key_acc, value_acc), grad_q)
        start = (jnp.zeros((NQB, BLK, HD), jnp.float32), jnp.zeros((NQB, BLK, HD), jnp.float32))
        inputs = (q_head, do_head, indices[head].astype(jnp.int32), valid[head] > 0, jnp.arange(NQB, dtype=jnp.int32))
        (key_acc, value_acc), grad_q = lax.scan(step, start, inputs)
        return (grad_q, key_acc.astype(jnp.bfloat16), value_acc.astype(jnp.bfloat16))
    grad_q, grad_k, grad_v = lax.map(per_head, jnp.arange(KVH, dtype=jnp.int32))
    grad_queries = grad_q.transpose(1, 2, 0, 3, 4).reshape(SEQ_LEN, KVH, GQ, HD)
    grad_keys = grad_k.transpose(1, 2, 0, 3).reshape(SEQ_LEN, KVH, HD)
    grad_values = grad_v.transpose(1, 2, 0, 3).reshape(SEQ_LEN, KVH, HD)
    return (grad_queries, grad_keys, grad_values)
```

```python
import functools
import math

import jax
import jax.numpy as jnp
from jax import lax
from jax.experimental import pallas as pl
from jax.experimental.pallas import tpu as pltpu
from jax.sharding import PartitionSpec as P

BLK = 64
CAP = 4
MESH = pl.DeviceIdType.MESH
NEG = -1e30
NT = (((1,), (1,)), ((), ()))
F32 = jnp.float32
BF = jnp.bfloat16


def dot(a, b):
    return jnp.dot(a, b, preferred_element_type=F32)


def dot_nt(a, b):
    return lax.dot_general(a, b, NT, preferred_element_type=F32)


def log2(n):
    shift = n.bit_length() - 1
    assert 1 << shift == n
    return shift


def iota(shape, axis):
    return lax.broadcasted_iota(jnp.int32, shape, axis)


def kernel(
    cfg,
    q_ref, do_ref, k_ref, v_ref, idx_ref, val_ref,
    dq_ref, dk_ref, dv_ref,
    sel, qaug, qd, kv, oh, kt, stage, pool, wt,
    s_own, dp_own, s_rem, dp_rem, pd, xsend, xrecv, tsend, trecv, ox_send, ox_recv, acc,
    a_send, a_recv, f_send, f_recv, x_send, x_recv, t_send, t_recv, o_sem, r_sem, in_sem, stats,
):
    S, heads, nb, total, topk, width, supers, pre, nbuf = cfg
    me = lax.axis_index("seq")
    core = lax.axis_index("inner")
    mate = 1 - core
    chunk = CAP * BLK
    nrem = (S - 1) * chunk
    rows_b = BLK * heads
    own_rows = nb * BLK
    lanes = sel.shape[1]
    slot_lanes = oh.shape[1]
    scaling = 1.0 / math.sqrt(width)
    c2 = scaling * math.log2(math.e)

    barrier = pltpu.get_barrier_semaphore()

    def hello(j, _):
        pl.semaphore_signal(
            barrier, inc=1, device_id={"seq": lax.rem(me + 1 + j, S)}, device_id_type=MESH
        )
        return 0

    lax.fori_loop(0, S - 1, hello, 0)
    pl.semaphore_signal(barrier, inc=1, device_id={"inner": mate}, device_id_type=MESH)

    loads = [
        pltpu.make_async_copy(src, dst, in_sem.at[i])
        for i, (src, dst) in enumerate(
            ((k_ref, kv.at[0]), (v_ref, kv.at[1]), (q_ref, qd.at[0]), (do_ref, qd.at[1]))
        )
    ]
    for load in loads:
        load.start()
    picked = jnp.where(val_ref[...] > 0, idx_ref[...], -1)
    block = iota((lanes, total), 0)
    hit = jnp.zeros((lanes, total), F32)
    for t in range(topk):
        hit = jnp.where(picked[t : t + 1, :] == block, 1.0, hit)
    eye = jnp.where(iota((total, total), 0) == iota((total, total), 1), 1.0, 0.0).astype(BF)
    sel[...] = dot_nt(eye, hit.astype(BF))
    nb_shift = log2(nb)
    tri_r = iota((lanes, lanes), 0)
    tri_c = iota((lanes, lanes), 1)
    tri = jnp.where(
        (tri_r < tri_c)
        & (lax.shift_right_logical(tri_r, nb_shift) == lax.shift_right_logical(tri_c, nb_shift)),
        1.0,
        0.0,
    ).astype(BF)

    def ranks(run):
        rows = sel[pl.ds(pl.multiple_of(run * nb, nb), nb), :]
        present = jnp.max(rows, axis=0, keepdims=True)
        rank = dot(jnp.broadcast_to(present, (8, lanes)).astype(BF), tri)[0:1, :]
        return rows, present, rank

    loads[0].wait()
    loads[1].wait()
    pl.semaphore_wait(barrier, S)

    def expand(axis):
        shape = (lanes, own_rows) if axis else (own_rows, lanes)
        block = lax.shift_right_logical(iota(shape, axis), log2(BLK)) + me * nb
        return jnp.where(block == iota(shape, 1 - axis), 1.0, 0.0).astype(BF)

    spread = expand(1)
    spread_t = expand(0)

    def send_a(r):
        return pltpu.make_async_remote_copy(
            src_ref=stage.at[r],
            dst_ref=pool.at[core, pl.ds(pl.multiple_of(me * chunk, chunk), chunk)],
            send_sem=a_send.at[r],
            recv_sem=a_recv.at[me],
            device_id={"seq": r},
            device_id_type=MESH,
        )

    def code_of(r):
        _, present, rank = ranks(r)
        return jnp.broadcast_to(jnp.where(present > 0.5, rank, -8.0), (8, lanes)).astype(BF)

    def scatter_of(code):
        down = dot_nt(spread_t, jnp.broadcast_to(code[0:1, :], (chunk, lanes)))
        down = down.astype(jnp.int32) * BLK + (iota((own_rows, chunk), 0) & (BLK - 1))
        return jnp.where(down == iota((own_rows, chunk), 1), 1.0, 0.0).astype(BF)

    def give(j, _):
        r = S - 1 - j
        code = code_of(r)
        across = dot(code, spread)[0:1, :].astype(jnp.int32) * BLK
        across = across + (iota((1, own_rows), 1) & (BLK - 1))
        pick = jnp.where(across == iota((chunk, own_rows), 0), 1.0, 0.0).astype(BF)
        stage[r] = dot(pick, kv[core]).astype(BF)
        send_a(r).start()
        if pre:
            wt[r] = scatter_of(code)
        return 0

    lax.fori_loop(0, S - 1 - me, give, 0)

    mine, present, rank = ranks(me)
    block_row = iota((1, lanes), 1)
    run_row = lax.shift_right_logical(block_row, nb_shift)
    place = jnp.where(
        run_row < me,
        run_row * CAP + rank.astype(jnp.int32),
        (S - 1) * CAP + (block_row & (nb - 1)),
    )
    place = jnp.where((present > 0.5) & (run_row <= me), place, -1)
    table = jnp.where(place == iota((slot_lanes, lanes), 0), 1.0, 0.0).astype(BF)
    bias = jnp.where(dot_nt(mine.astype(BF), table) > 0.5, 0.0, NEG)
    loads[2].wait()
    loads[3].wait()
    for b in range(nb):
        rows = pl.ds(b * rows_b, rows_b)
        qaug[rows, 0:width] = qd[0, rows, :]
        qaug[rows, width:] = jnp.broadcast_to(bias[b : b + 1, :], (rows_b, slot_lanes)).astype(BF)
    nkeys = oh.shape[0]
    oh[...] = jnp.where(
        lax.shift_right_logical(iota((nkeys, slot_lanes), 0), log2(BLK))
        == iota((nkeys, slot_lanes), 1),
        1.0,
        0.0,
    ).astype(BF)
    kt[:, nrem:] = kv[0].astype(F32).T.astype(BF)

    pair = 2 if nb % 2 == 0 else 1

    def own_count(b):
        return (b // pair + 1) * pair * BLK

    def own_scores(b, at):
        n = own_count(b)
        rows = pl.ds(b * rows_b, rows_b)
        ka = jnp.concatenate([kv[0, 0:n, :], oh[nrem : nrem + n, :]], axis=1)
        s = dot_nt(ka, qaug[rows, :])
        key = iota((n, rows_b), 0) - b * BLK
        query = lax.shift_right_logical(iota((n, rows_b), 1), log2(heads))
        s_own[at, 0:n, :] = jnp.where(key > query, NEG, s)
        dp_own[at, 0:n, :] = dot_nt(kv[1, 0:n, :], qd[1, rows, :])

    def fold(x, how):
        return how(x.reshape(-1, 8, rows_b), axis=0)

    if pre:
        for b in range(nb):
            own_scores(b, b)

    def blank(s, _):
        at = pl.ds(pl.multiple_of(s * chunk, chunk), chunk)
        pool[0, at, :] = jnp.zeros((chunk, width), BF)
        pool[1, at, :] = jnp.zeros((chunk, width), BF)
        return 0

    lax.fori_loop(me, S - 1, blank, 0)

    def pool_at(kind, s):
        return pool.at[kind, pl.ds(pl.multiple_of(s * chunk, chunk), chunk)]

    def recv_a(s):
        return pltpu.make_async_remote_copy(
            src_ref=stage.at[s],
            dst_ref=pool_at(core, s),
            send_sem=a_send.at[s],
            recv_sem=a_recv.at[s],
            device_id={"seq": s},
            device_id_type=MESH,
        )

    def forward(kind, s):
        return pltpu.make_async_remote_copy(
            src_ref=pool_at(kind, s),
            dst_ref=pool_at(kind, s),
            send_sem=f_send.at[s],
            recv_sem=f_recv.at[s],
            device_id={"inner": mate},
            device_id_type=MESH,
        )

    def pass_on(j, _):
        s = me - 1 - j
        recv_a(s).wait_recv()
        forward(core, s).start()
        return 0

    lax.fori_loop(0, me, pass_on, 0)

    def take(j, _):
        s = me - 1 - j
        forward(mate, s).wait_recv()
        return 0

    lax.fori_loop(0, me, take, 0)

    step = nrem // supers

    def loop(body, init):
        for j in range(supers):
            init = body(j, init)
        return init

    def span(j):
        return pl.ds(j * step, step)

    for s in range(S - 1):
        kt[:, s * chunk : (s + 1) * chunk] = (
            pool[0, s * chunk : (s + 1) * chunk, :].astype(F32).T.astype(BF)
        )

    def third_on(s_view, dp_view, where, rows, keys_at, inv, delta):
        p = s_view[where] * inv
        pd[1, keys_at, rows] = p.astype(BF)
        pd[0, keys_at, rows] = (p * (dp_view[where] - delta)).astype(BF)

    for b in range(nb):
        at = b if pre else 0
        buf = b % nbuf
        n = own_count(b)
        rows = pl.ds(b * rows_b, rows_b)
        if not pre:
            own_scores(b, 0)
        qa = qaug[rows, :]
        dob = qd[1, rows, :]

        def first(j, m):
            here = span(j)
            ka = jnp.concatenate([pool[0, here, :], oh[here, :]], axis=1)
            s = dot_nt(ka, qa)
            s_rem[buf, here, :] = s
            dp_rem[buf, here, :] = dot_nt(pool[1, here, :], dob)
            return jnp.maximum(m, fold(s, jnp.max))

        m = loop(first, fold(s_own[at, 0:n, :], jnp.max))
        m = jnp.max(m, axis=0, keepdims=True)

        def second_on(s_view, dp_view, where, carry):
            l, d = carry
            e = jnp.exp2((s_view[where] - m) * c2)
            s_view[where] = e
            return (
                l + fold(e, jnp.sum),
                d + fold(e * dp_view[where], jnp.sum),
            )

        zero = jnp.zeros((8, rows_b), F32)
        carry = second_on(s_own, dp_own, (at, slice(0, n)), (zero, zero))
        l, d = loop(lambda j, c: second_on(s_rem, dp_rem, (buf, span(j)), c), carry)
        inv = 1.0 / jnp.sum(l, axis=0, keepdims=True)
        delta = jnp.sum(d, axis=0, keepdims=True) * inv

        if pre:
            stats[b, 0:1, :] = inv
            stats[b, 1:2, :] = delta
        else:
            third_on(s_own, dp_own, (at, slice(0, n)), rows, pl.ds(nrem, n), inv, delta)

        def third(j, c):
            third_on(s_rem, dp_rem, (buf, span(j)), rows, span(j), inv, delta)
            return c

        loop(third, 0)

    def scale_of(kind):
        return jnp.where(kind == 0, scaling, 1.0).astype(F32)

    def remote_terms(kind, s):
        at = pl.ds(pl.multiple_of(s * chunk, chunk), chunk)
        return dot(pd[kind, at, :], qd[kind]) * scale_of(kind)

    def swap(s):
        return pltpu.make_async_remote_copy(
            src_ref=xsend.at[s],
            dst_ref=xrecv.at[s],
            send_sem=x_send.at[s],
            recv_sem=x_recv.at[s],
            device_id={"inner": mate},
            device_id_type=MESH,
        )

    def give_back(s):
        return pltpu.make_async_remote_copy(
            src_ref=tsend.at[s],
            dst_ref=trecv.at[me],
            send_sem=t_send.at[s],
            recv_sem=t_recv.at[me],
            device_id={"seq": s},
            device_id_type=MESH,
        )

    def other(s, _):
        xsend[s] = remote_terms(mate, s)
        swap(s).start()
        return 0

    lax.fori_loop(0, jnp.minimum(me, 1), other, 0)

    def ours(s, _):
        @pl.when(s + 1 < me)
        def _():
            other(s + 1, 0)

        total_terms = remote_terms(core, s)
        swap(s).wait_recv()
        tsend[s] = (total_terms + xrecv[s]).astype(BF)
        give_back(s).start()
        return 0

    lax.fori_loop(0, me, ours, 0)

    own_swap = pltpu.make_async_remote_copy(
        src_ref=ox_send,
        dst_ref=ox_recv,
        send_sem=o_sem.at[0],
        recv_sem=o_sem.at[1],
        device_id={"inner": mate},
        device_id_type=MESH,
    )

    def own_terms(kind, target):
        for c in range(0, nb, pair):
            n = pair * BLK
            lo = c * rows_b
            target[c * BLK : c * BLK + n, :] = (
                dot(pd[kind, nrem + c * BLK : nrem + c * BLK + n, lo:], qd[kind, lo:, :])
                * scale_of(kind)
            )

    if pre:
        for b in range(nb):
            n = own_count(b)
            third_on(
                s_own, dp_own, (b, slice(0, n)), pl.ds(b * rows_b, rows_b), pl.ds(nrem, n),
                stats[b, 0:1, :], stats[b, 1:2, :],
            )
    own_terms(mate, ox_send)
    own_swap.start()
    own_terms(core, acc)

    for b in range(nb):
        rows = pl.ds(b * rows_b, rows_b)
        n = nrem + own_count(b)
        turned = dot(kt[:, 0:n], pd[0, 0:n, rows]) * scaling
        dq_ref[rows, :] = turned.T.astype(BF)

    own_swap.wait_recv()
    acc[...] += ox_recv[...]

    def gather(j, _):
        r = me + 1 + j
        pltpu.make_async_remote_copy(
            src_ref=tsend.at[r],
            dst_ref=trecv.at[r],
            send_sem=t_send.at[r],
            recv_sem=t_recv.at[r],
            device_id={"seq": r},
            device_id_type=MESH,
        ).wait_recv()
        acc[...] += dot(wt[r] if pre else scatter_of(code_of(r)), trecv[r])
        return 0

    lax.fori_loop(0, S - 1 - me, gather, 0)

    def last(ref):
        return pltpu.make_async_remote_copy(
            src_ref=ref,
            dst_ref=ref,
            send_sem=r_sem.at[0],
            recv_sem=r_sem.at[1],
            device_id={"inner": mate},
            device_id_type=MESH,
        )

    @pl.when(core == 0)
    def _():
        dk_ref[...] = acc[...].astype(BF)
        last(dk_ref).start()

    @pl.when(core == 1)
    def _():
        dv_ref[...] = acc[...].astype(BF)
        last(dv_ref).start()

    def close_up(j, _):
        send_a(me + 1 + j).wait_send()
        return 0

    lax.fori_loop(0, S - 1 - me, close_up, 0)

    def close_down(s, _):
        forward(core, s).wait_send()
        swap(s).wait_send()
        give_back(s).wait_send()
        return 0

    lax.fori_loop(0, me, close_down, 0)
    own_swap.wait_send()

    @pl.when(core == 0)
    def _():
        last(dk_ref).wait_send()
        last(dv_ref).wait_recv()

    @pl.when(core == 1)
    def _():
        last(dv_ref).wait_send()
        last(dk_ref).wait_recv()


def place_kernel(*refs):
    n = len(refs) // 2
    moves = [pltpu.make_async_copy(refs[i], refs[n + i], refs[-1].at[i]) for i in range(n)]
    for move in moves:
        move.start()
    for move in moves:
        move.wait()


def place(*arrays):
    return pl.pallas_call(
        place_kernel,
        out_shape=tuple(jax.ShapeDtypeStruct(a.shape, a.dtype) for a in arrays),
        in_specs=[pl.BlockSpec(memory_space=pltpu.VMEM)] * len(arrays),
        out_specs=(pl.BlockSpec(memory_space=pl.ANY),) * len(arrays),
        scratch_shapes=[pltpu.SemaphoreType.DMA((len(arrays),))],
        compiler_params=pltpu.CompilerParams(vmem_limit_bytes=65536),
    )(*(pltpu.with_memory_space_constraint(a, pltpu.VMEM) for a in arrays))


def per_device(queries, grad_out, keys, values, indices, valid):
    tokens, _, heads, width = queries.shape
    S = lax.axis_size("seq")
    total, topk = indices.shape[1:]
    nb = tokens // BLK
    chunk = CAP * BLK
    nrem = (S - 1) * chunk
    own_rows = tokens
    nkeys = nrem + own_rows
    rows = tokens * heads
    rows_b = BLK * heads
    lanes = -(-total // 128) * 128
    slot_lanes = -(-(nkeys // BLK) // 128) * 128
    supers = next(n for n in range(1, S) if (S - 1) % n == 0 and (S - 1) // n <= 4)
    pre = supers == 1
    nbuf = 2 if pre else 1
    n_own = nb if pre else 1
    cfg = (S, heads, nb, total, topk, width, supers, pre, nbuf)
    vmem = pl.BlockSpec(memory_space=pltpu.VMEM)
    hbm = pl.BlockSpec(memory_space=pl.ANY)
    dma = pltpu.SemaphoreType.DMA
    dq, dk, dv = pl.pallas_call(
        functools.partial(kernel, cfg),
        out_shape=(
            pltpu.VMEM((rows, width), BF),
            pltpu.VMEM((own_rows, width), BF),
            pltpu.VMEM((own_rows, width), BF),
        ),
        in_specs=[hbm] * 4 + [vmem] * 2,
        out_specs=(vmem, vmem, vmem),
        scratch_shapes=[
            pltpu.VMEM((total, lanes), F32),
            pltpu.VMEM((rows, width + slot_lanes), BF),
            pltpu.VMEM((2, rows, width), BF),
            pltpu.VMEM((2, own_rows, width), BF),
            pltpu.VMEM((nkeys, slot_lanes), BF),
            pltpu.VMEM((width, nkeys), BF),
            pltpu.VMEM((S, chunk, width), BF),
            pltpu.VMEM((2, nrem, width), BF),
            pltpu.VMEM((S if pre else 1, own_rows, chunk), BF),
            pltpu.VMEM((n_own, own_rows, rows_b), F32),
            pltpu.VMEM((n_own, own_rows, rows_b), F32),
            pltpu.VMEM((nbuf, nrem, rows_b), F32),
            pltpu.VMEM((nbuf, nrem, rows_b), F32),
            pltpu.VMEM((2, nkeys, rows), BF),
            pltpu.VMEM((S, chunk, width), F32),
            pltpu.VMEM((S, chunk, width), F32),
            pltpu.VMEM((S, chunk, width), BF),
            pltpu.VMEM((S, chunk, width), BF),
            pltpu.VMEM((own_rows, width), F32),
            pltpu.VMEM((own_rows, width), F32),
            pltpu.VMEM((own_rows, width), F32),
            dma((S,)), dma((S,)), dma((S,)), dma((S,)), dma((S,)), dma((S,)),
            dma((S,)), dma((S,)), dma((2,)), dma((2,)),
            dma((5,)),
            pltpu.VMEM((nb, 2, rows_b), F32),
        ],
        compiler_params=pltpu.CompilerParams(
            collective_id=0, has_side_effects=True, vmem_limit_bytes=67043328 - 6 * own_rows * width * 2 - 4096
        ),
    )(
        queries.reshape(rows, width),
        grad_out.reshape(rows, width),
        keys.reshape(own_rows, width),
        values.reshape(own_rows, width),
        indices[0].T,
        valid[0].T,
    )
    dq, dk, dv = place(dq, dk, dv)
    return (
        dq.reshape(tokens, 1, heads, width),
        dk.reshape(tokens, 1, width),
        dv.reshape(tokens, 1, width),
    )


def solution(mesh):
    return jax.shard_map(
        per_device,
        mesh=mesh,
        in_specs=(
            P(("groups", "seq"), "head", "inner", None),
            P(("groups", "seq"), "head", "inner", None),
            P(("groups", "seq"), "head", None),
            P(("groups", "seq"), "head", None),
            P("head", "groups", None),
            P("head", "groups", None),
        ),
        out_specs=(
            P(("groups", "seq"), "head", "inner", None),
            P(("groups", "seq"), "head", None),
            P(("groups", "seq"), "head", None),
        ),
        check_vma=False,
    )
```

```python
import functools
import math

import jax
import jax.numpy as jnp
from jax import lax
from jax.experimental import pallas as pl
from jax.experimental.pallas import tpu as pltpu
from jax.sharding import PartitionSpec as P

BLK = 64
CAP = 4
MESH = pl.DeviceIdType.MESH
NEG = -1e30
NT = (((1,), (1,)), ((), ()))
F32 = jnp.float32
BF = jnp.bfloat16


def dot(a, b):
    return jnp.dot(a, b, preferred_element_type=F32)


def dot_nt(a, b):
    return lax.dot_general(a, b, NT, preferred_element_type=F32)


def log2(n):
    shift = n.bit_length() - 1
    assert 1 << shift == n
    return shift


def iota(shape, axis):
    return lax.broadcasted_iota(jnp.int32, shape, axis)


def kernel(
    cfg,
    q_ref, do_ref, k_ref, v_ref, idx_hbm, val_hbm,
    dq_ref, dk_ref, dv_ref,
    sel, qaug, qd, kv, oh, kt, stage, pool, wt,
    s_own, dp_own, s_rem, dp_rem, pd, xsend, xrecv, tsend, trecv, ox_send, ox_recv, acc,
    a_send, a_recv, f_send, f_recv, x_send, x_recv, t_send, t_recv, o_sem, r_sem, in_sem, stats,
    ready, slots,
):
    S, heads, nb, total, topk, width, supers, pre, nbuf = cfg
    me = lax.axis_index("seq")
    core = lax.axis_index("inner")
    mate = 1 - core
    chunk = CAP * BLK
    nrem = (S - 1) * chunk
    rows_b = BLK * heads
    own_rows = nb * BLK
    lanes = sel.shape[1]
    slot_lanes = oh.shape[1]
    scaling = 1.0 / math.sqrt(width)
    c2 = scaling * math.log2(math.e)

    barrier = pltpu.get_barrier_semaphore()

    def hello(j, _):
        pl.semaphore_signal(barrier, inc=1, device_id={"seq": S - 1 - j}, device_id_type=MESH)
        return 0

    lax.fori_loop(0, S - 1 - me, hello, 0)
    pl.semaphore_signal(barrier, inc=1, device_id={"inner": mate}, device_id_type=MESH)

    loads = [
        pltpu.make_async_copy(src, dst, in_sem.at[i])
        for i, (src, dst) in enumerate(
            (
                (idx_hbm, slots.at[0]), (val_hbm, slots.at[1]),
                (k_ref, kv.at[0]), (v_ref, kv.at[1]), (q_ref, qd.at[0]), (do_ref, qd.at[1]),
            )
        )
    ]
    for load in loads:
        load.start()

    pl.semaphore_wait(barrier, me + 1)

    def answer(j, _):
        pl.semaphore_signal(ready.at[me], inc=1, device_id={"seq": j}, device_id_type=MESH)
        return 0

    lax.fori_loop(0, me, answer, 0)

    loads[0].wait()
    loads[1].wait()
    picked = jnp.where(slots[1] > 0, slots[0], -1)
    block = iota((lanes, total), 0)
    hit = jnp.zeros((lanes, total), F32)
    for t in range(topk):
        hit = jnp.where(picked[t : t + 1, :] == block, 1.0, hit)
    eye = jnp.where(iota((total, total), 0) == iota((total, total), 1), 1.0, 0.0).astype(BF)
    sel[...] = dot_nt(eye, hit.astype(BF))
    nb_shift = log2(nb)
    tri_r = iota((lanes, lanes), 0)
    tri_c = iota((lanes, lanes), 1)
    tri = jnp.where(
        (tri_r < tri_c)
        & (lax.shift_right_logical(tri_r, nb_shift) == lax.shift_right_logical(tri_c, nb_shift)),
        1.0,
        0.0,
    ).astype(BF)

    def ranks(run):
        rows = sel[pl.ds(pl.multiple_of(run * nb, nb), nb), :]
        present = jnp.max(rows, axis=0, keepdims=True)
        rank = dot(jnp.broadcast_to(present, (8, lanes)).astype(BF), tri)[0:1, :]
        return rows, present, rank

    def expand(axis):
        shape = (lanes, own_rows) if axis else (own_rows, lanes)
        block = lax.shift_right_logical(iota(shape, axis), log2(BLK)) + me * nb
        return jnp.where(block == iota(shape, 1 - axis), 1.0, 0.0).astype(BF)

    spread = expand(1)
    spread_t = expand(0)

    def send_a(r):
        return pltpu.make_async_remote_copy(
            src_ref=stage.at[r],
            dst_ref=pool.at[core, pl.ds(pl.multiple_of(me * chunk, chunk), chunk)],
            send_sem=a_send.at[r],
            recv_sem=a_recv.at[me],
            device_id={"seq": r},
            device_id_type=MESH,
        )

    def code_of(r):
        _, present, rank = ranks(r)
        return jnp.broadcast_to(jnp.where(present > 0.5, rank, -8.0), (8, lanes)).astype(BF)

    def scatter_of(code):
        down = dot_nt(spread_t, jnp.broadcast_to(code[0:1, :], (chunk, lanes)))
        down = down.astype(jnp.int32) * BLK + (iota((own_rows, chunk), 0) & (BLK - 1))
        return jnp.where(down == iota((own_rows, chunk), 1), 1.0, 0.0).astype(BF)

    loads[2].wait()
    loads[3].wait()

    def give(j, _):
        r = me + 1 + j
        code = code_of(r)
        across = dot(code, spread)[0:1, :].astype(jnp.int32) * BLK
        across = across + (iota((1, own_rows), 1) & (BLK - 1))
        pick = jnp.where(across == iota((chunk, own_rows), 0), 1.0, 0.0).astype(BF)
        stage[r] = dot(pick, kv[core]).astype(BF)
        pl.semaphore_wait(ready.at[r], 1)
        send_a(r).start()
        return 0

    lax.fori_loop(0, S - 1 - me, give, 0)

    mine, present, rank = ranks(me)
    block_row = iota((1, lanes), 1)
    run_row = lax.shift_right_logical(block_row, nb_shift)
    place = jnp.where(
        run_row < me,
        run_row * CAP + rank.astype(jnp.int32),
        (S - 1) * CAP + (block_row & (nb - 1)),
    )
    place = jnp.where((present > 0.5) & (run_row <= me), place, -1)
    table = jnp.where(place == iota((slot_lanes, lanes), 0), 1.0, 0.0).astype(BF)
    bias = jnp.where(dot_nt(mine.astype(BF), table) > 0.5, 0.0, NEG)
    loads[4].wait()
    loads[5].wait()
    for b in range(nb):
        rows = pl.ds(b * rows_b, rows_b)
        qaug[rows, 0:width] = qd[0, rows, :]
        qaug[rows, width:] = jnp.broadcast_to(bias[b : b + 1, :], (rows_b, slot_lanes)).astype(BF)
    nkeys = oh.shape[0]
    oh[...] = jnp.where(
        lax.shift_right_logical(iota((nkeys, slot_lanes), 0), log2(BLK))
        == iota((nkeys, slot_lanes), 1),
        1.0,
        0.0,
    ).astype(BF)
    kt[:, nrem:] = kv[0].astype(F32).T.astype(BF)

    pair = 2 if nb % 2 == 0 else 1

    def own_count(b):
        return (b // pair + 1) * pair * BLK

    def own_scores(b, at):
        n = own_count(b)
        rows = pl.ds(b * rows_b, rows_b)
        ka = jnp.concatenate([kv[0, 0:n, :], oh[nrem : nrem + n, :]], axis=1)
        s = dot_nt(ka, qaug[rows, :])
        key = iota((n, rows_b), 0) - b * BLK
        query = lax.shift_right_logical(iota((n, rows_b), 1), log2(heads))
        s_own[at, 0:n, :] = jnp.where(key > query, NEG, s)
        dp_own[at, 0:n, :] = dot_nt(kv[1, 0:n, :], qd[1, rows, :])

    def fold(x, how):
        return how(x.reshape(-1, 8, rows_b), axis=0)

    if pre:
        for b in range(nb):
            own_scores(b, b)

    if pre:

        def scatters(j, _):
            r = me + 1 + j
            wt[r] = scatter_of(code_of(r))
            return 0

        lax.fori_loop(0, S - 1 - me, scatters, 0)

    def blank(s, _):
        at = pl.ds(pl.multiple_of(s * chunk, chunk), chunk)
        pool[0, at, :] = jnp.zeros((chunk, width), BF)
        pool[1, at, :] = jnp.zeros((chunk, width), BF)
        return 0

    lax.fori_loop(me, S - 1, blank, 0)

    def pool_at(kind, s):
        return pool.at[kind, pl.ds(pl.multiple_of(s * chunk, chunk), chunk)]

    def recv_a(s):
        return pltpu.make_async_remote_copy(
            src_ref=stage.at[s],
            dst_ref=pool_at(core, s),
            send_sem=a_send.at[s],
            recv_sem=a_recv.at[s],
            device_id={"seq": s},
            device_id_type=MESH,
        )

    def forward(kind, s):
        return pltpu.make_async_remote_copy(
            src_ref=pool_at(kind, s),
            dst_ref=pool_at(kind, s),
            send_sem=f_send.at[s],
            recv_sem=f_recv.at[s],
            device_id={"inner": mate},
            device_id_type=MESH,
        )

    def pass_on(j, _):
        s = me - 1 - j
        recv_a(s).wait_recv()
        forward(core, s).start()
        return 0

    lax.fori_loop(0, me, pass_on, 0)

    def take(j, _):
        s = me - 1 - j
        forward(mate, s).wait_recv()
        return 0

    lax.fori_loop(0, me, take, 0)

    step = nrem // supers

    def loop(body, init):
        for j in range(supers):
            init = body(j, init)
        return init

    def span(j):
        return pl.ds(j * step, step)

    for s in range(S - 1):
        kt[:, s * chunk : (s + 1) * chunk] = (
            pool[0, s * chunk : (s + 1) * chunk, :].astype(F32).T.astype(BF)
        )

    def third_on(s_view, dp_view, where, rows, keys_at, inv, delta):
        p = s_view[where] * inv
        pd[1, keys_at, rows] = p.astype(BF)
        pd[0, keys_at, rows] = (p * (dp_view[where] - delta)).astype(BF)

    for b in range(nb):
        at = b if pre else 0
        buf = b % nbuf
        n = own_count(b)
        rows = pl.ds(b * rows_b, rows_b)
        if not pre:
            own_scores(b, 0)
        qa = qaug[rows, :]
        dob = qd[1, rows, :]

        def first(j, m):
            here = span(j)
            ka = jnp.concatenate([pool[0, here, :], oh[here, :]], axis=1)
            s = dot_nt(ka, qa)
            s_rem[buf, here, :] = s
            dp_rem[buf, here, :] = dot_nt(pool[1, here, :], dob)
            return jnp.maximum(m, fold(s, jnp.max))

        m = loop(first, fold(s_own[at, 0:n, :], jnp.max))
        m = jnp.max(m, axis=0, keepdims=True)

        def second_on(s_view, dp_view, where, carry):
            l, d = carry
            e = jnp.exp2((s_view[where] - m) * c2)
            s_view[where] = e
            return (
                l + fold(e, jnp.sum),
                d + fold(e * dp_view[where], jnp.sum),
            )

        zero = jnp.zeros((8, rows_b), F32)
        carry = second_on(s_own, dp_own, (at, slice(0, n)), (zero, zero))
        l, d = loop(lambda j, c: second_on(s_rem, dp_rem, (buf, span(j)), c), carry)
        inv = 1.0 / jnp.sum(l, axis=0, keepdims=True)
        delta = jnp.sum(d, axis=0, keepdims=True) * inv

        if pre:
            stats[b, 0:1, :] = inv
            stats[b, 1:2, :] = delta
        else:
            third_on(s_own, dp_own, (at, slice(0, n)), rows, pl.ds(nrem, n), inv, delta)

        def third(j, c):
            third_on(s_rem, dp_rem, (buf, span(j)), rows, span(j), inv, delta)
            return c

        loop(third, 0)

    def scale_of(kind):
        return jnp.where(kind == 0, scaling, 1.0).astype(F32)

    def remote_terms(kind, s):
        at = pl.ds(pl.multiple_of(s * chunk, chunk), chunk)
        return dot(pd[kind, at, :], qd[kind]) * scale_of(kind)

    def swap(s):
        return pltpu.make_async_remote_copy(
            src_ref=xsend.at[s],
            dst_ref=xrecv.at[s],
            send_sem=x_send.at[s],
            recv_sem=x_recv.at[s],
            device_id={"inner": mate},
            device_id_type=MESH,
        )

    def give_back(s):
        return pltpu.make_async_remote_copy(
            src_ref=tsend.at[s],
            dst_ref=trecv.at[me],
            send_sem=t_send.at[s],
            recv_sem=t_recv.at[me],
            device_id={"seq": s},
            device_id_type=MESH,
        )

    def other(s, _):
        xsend[s] = remote_terms(mate, s)
        swap(s).start()
        return 0

    lax.fori_loop(0, jnp.minimum(me, 1), other, 0)

    def ours(s, _):
        @pl.when(s + 1 < me)
        def _():
            other(s + 1, 0)

        total_terms = remote_terms(core, s)
        swap(s).wait_recv()
        tsend[s] = (total_terms + xrecv[s]).astype(BF)
        give_back(s).start()
        return 0

    lax.fori_loop(0, me, ours, 0)

    own_swap = pltpu.make_async_remote_copy(
        src_ref=ox_send,
        dst_ref=ox_recv,
        send_sem=o_sem.at[0],
        recv_sem=o_sem.at[1],
        device_id={"inner": mate},
        device_id_type=MESH,
    )

    def own_terms(kind, target):
        for c in range(0, nb, pair):
            n = pair * BLK
            lo = c * rows_b
            target[c * BLK : c * BLK + n, :] = (
                dot(pd[kind, nrem + c * BLK : nrem + c * BLK + n, lo:], qd[kind, lo:, :])
                * scale_of(kind)
            )

    if pre:
        for b in range(nb):
            n = own_count(b)
            third_on(
                s_own, dp_own, (b, slice(0, n)), pl.ds(b * rows_b, rows_b), pl.ds(nrem, n),
                stats[b, 0:1, :], stats[b, 1:2, :],
            )
    own_terms(mate, ox_send)
    own_swap.start()
    own_terms(core, acc)

    for b in range(nb):
        rows = pl.ds(b * rows_b, rows_b)
        n = nrem + own_count(b)
        turned = dot(kt[:, 0:n], pd[0, 0:n, rows]) * scaling
        dq_ref[rows, :] = turned.T.astype(BF)

    own_swap.wait_recv()
    acc[...] += ox_recv[...]

    def gather(j, _):
        r = me + 1 + j
        pltpu.make_async_remote_copy(
            src_ref=tsend.at[r],
            dst_ref=trecv.at[r],
            send_sem=t_send.at[r],
            recv_sem=t_recv.at[r],
            device_id={"seq": r},
            device_id_type=MESH,
        ).wait_recv()
        acc[...] += dot(wt[r] if pre else scatter_of(code_of(r)), trecv[r])
        return 0

    lax.fori_loop(0, S - 1 - me, gather, 0)

    def last(ref):
        return pltpu.make_async_remote_copy(
            src_ref=ref,
            dst_ref=ref,
            send_sem=r_sem.at[0],
            recv_sem=r_sem.at[1],
            device_id={"inner": mate},
            device_id_type=MESH,
        )

    @pl.when(core == 0)
    def _():
        dk_ref[...] = acc[...].astype(BF)
        last(dk_ref).start()

    @pl.when(core == 1)
    def _():
        dv_ref[...] = acc[...].astype(BF)
        last(dv_ref).start()

    def close_up(j, _):
        send_a(me + 1 + j).wait_send()
        return 0

    lax.fori_loop(0, S - 1 - me, close_up, 0)

    def close_down(s, _):
        forward(core, s).wait_send()
        swap(s).wait_send()
        give_back(s).wait_send()
        return 0

    lax.fori_loop(0, me, close_down, 0)
    own_swap.wait_send()

    @pl.when(core == 0)
    def _():
        last(dk_ref).wait_send()
        last(dv_ref).wait_recv()

    @pl.when(core == 1)
    def _():
        last(dv_ref).wait_send()
        last(dk_ref).wait_recv()


def place_kernel(*refs):
    n = len(refs) // 2
    moves = [pltpu.make_async_copy(refs[i], refs[n + i], refs[-1].at[i]) for i in range(n)]
    for move in moves:
        move.start()
    for move in moves:
        move.wait()


def place(*arrays):
    return pl.pallas_call(
        place_kernel,
        out_shape=tuple(jax.ShapeDtypeStruct(a.shape, a.dtype) for a in arrays),
        in_specs=[pl.BlockSpec(memory_space=pltpu.VMEM)] * len(arrays),
        out_specs=(pl.BlockSpec(memory_space=pl.ANY),) * len(arrays),
        scratch_shapes=[pltpu.SemaphoreType.DMA((len(arrays),))],
        compiler_params=pltpu.CompilerParams(vmem_limit_bytes=65536),
    )(*(pltpu.with_memory_space_constraint(a, pltpu.VMEM) for a in arrays))


def per_device(queries, grad_out, keys, values, indices, valid):
    tokens, _, heads, width = queries.shape
    S = lax.axis_size("seq")
    total, topk = indices.shape[1:]
    nb = tokens // BLK
    chunk = CAP * BLK
    nrem = (S - 1) * chunk
    own_rows = tokens
    nkeys = nrem + own_rows
    rows = tokens * heads
    rows_b = BLK * heads
    lanes = -(-total // 128) * 128
    slot_lanes = -(-(nkeys // BLK) // 128) * 128
    supers = next(n for n in range(1, S) if (S - 1) % n == 0 and (S - 1) // n <= 4)
    pre = supers == 1
    nbuf = 2 if pre else 1
    n_own = nb if pre else 1
    cfg = (S, heads, nb, total, topk, width, supers, pre, nbuf)
    vmem = pl.BlockSpec(memory_space=pltpu.VMEM)
    hbm = pl.BlockSpec(memory_space=pl.ANY)
    dma = pltpu.SemaphoreType.DMA
    dq, dk, dv = pl.pallas_call(
        functools.partial(kernel, cfg),
        out_shape=(
            pltpu.VMEM((rows, width), BF),
            pltpu.VMEM((own_rows, width), BF),
            pltpu.VMEM((own_rows, width), BF),
        ),
        in_specs=[hbm] * 6,
        out_specs=(vmem, vmem, vmem),
        scratch_shapes=[
            pltpu.VMEM((total, lanes), F32),
            pltpu.VMEM((rows, width + slot_lanes), BF),
            pltpu.VMEM((2, rows, width), BF),
            pltpu.VMEM((2, own_rows, width), BF),
            pltpu.VMEM((nkeys, slot_lanes), BF),
            pltpu.VMEM((width, nkeys), BF),
            pltpu.VMEM((S, chunk, width), BF),
            pltpu.VMEM((2, nrem, width), BF),
            pltpu.VMEM((S if pre else 1, own_rows, chunk), BF),
            pltpu.VMEM((n_own, own_rows, rows_b), F32),
            pltpu.VMEM((n_own, own_rows, rows_b), F32),
            pltpu.VMEM((nbuf, nrem, rows_b), F32),
            pltpu.VMEM((nbuf, nrem, rows_b), F32),
            pltpu.VMEM((2, nkeys, rows), BF),
            pltpu.VMEM((S, chunk, width), F32),
            pltpu.VMEM((S, chunk, width), F32),
            pltpu.VMEM((S, chunk, width), BF),
            pltpu.VMEM((S, chunk, width), BF),
            pltpu.VMEM((own_rows, width), F32),
            pltpu.VMEM((own_rows, width), F32),
            pltpu.VMEM((own_rows, width), F32),
            dma((S,)), dma((S,)), dma((S,)), dma((S,)), dma((S,)), dma((S,)),
            dma((S,)), dma((S,)), dma((2,)), dma((2,)),
            dma((6,)),
            pltpu.VMEM((nb, 2, rows_b), F32),
            pltpu.SemaphoreType.REGULAR((S,)),
            pltpu.VMEM((2, topk, total), jnp.int32),
        ],
        compiler_params=pltpu.CompilerParams(
            collective_id=0, has_side_effects=True, vmem_limit_bytes=67043328 - 6 * own_rows * width * 2 - 4096
        ),
    )(
        queries.reshape(rows, width),
        grad_out.reshape(rows, width),
        keys.reshape(own_rows, width),
        values.reshape(own_rows, width),
        indices[0].T,
        valid[0].T,
    )
    dq, dk, dv = place(dq, dk, dv)
    return (
        dq.reshape(tokens, 1, heads, width),
        dk.reshape(tokens, 1, width),
        dv.reshape(tokens, 1, width),
    )


def solution(mesh):
    return jax.shard_map(
        per_device,
        mesh=mesh,
        in_specs=(
            P(("groups", "seq"), "head", "inner", None),
            P(("groups", "seq"), "head", "inner", None),
            P(("groups", "seq"), "head", None),
            P(("groups", "seq"), "head", None),
            P("head", "groups", None),
            P("head", "groups", None),
        ),
        out_specs=(
            P(("groups", "seq"), "head", "inner", None),
            P(("groups", "seq"), "head", None),
            P(("groups", "seq"), "head", None),
        ),
        check_vma=False,
    )
```

```python
import functools
import math

import jax
import jax.numpy as jnp
from jax import lax
from jax.experimental import pallas as pl
from jax.experimental.pallas import tpu as pltpu
from jax.sharding import PartitionSpec as P

BLK = 64
CAP = 4
MESH = pl.DeviceIdType.MESH
NEG = -1e30
NT = (((1,), (1,)), ((), ()))
F32 = jnp.float32
BF = jnp.bfloat16


def dot(a, b):
    return jnp.dot(a, b, preferred_element_type=F32)


def dot_nt(a, b):
    return lax.dot_general(a, b, NT, preferred_element_type=F32)


def log2(n):
    shift = n.bit_length() - 1
    assert 1 << shift == n
    return shift


def iota(shape, axis):
    return lax.broadcasted_iota(jnp.int32, shape, axis)


def kernel(
    cfg,
    q_ref, do_ref, k_ref, v_ref, idx_hbm, val_hbm,
    dq_ref, dk_ref, dv_ref,
    sel, qaug, qd, kv, oh, kt, vt, vt_own, dot_t, stage, pool, wt,
    s_buf, pd, terms, xrecv, tsend, trecv, ox_send, ox_recv, acc,
    a_send, a_recv, f_send, f_recv, x_send, x_recv, t_send, t_recv, o_sem, r_sem, in_sem,
    ready, slots, st_m, st_l, st_d,
):
    S, heads, nb, total, topk, width, pre = cfg
    me = lax.axis_index("seq")
    core = lax.axis_index("inner")
    mate = 1 - core
    chunk = CAP * BLK
    nrem = (S - 1) * chunk
    rows_b = BLK * heads
    own_rows = nb * BLK
    lanes = sel.shape[1]
    slot_lanes = oh.shape[1]
    scaling = 1.0 / math.sqrt(width)
    c2 = scaling * math.log2(math.e)

    barrier = pltpu.get_barrier_semaphore()

    def hello(j, _):
        pl.semaphore_signal(barrier, inc=1, device_id={"seq": S - 1 - j}, device_id_type=MESH)
        return 0

    lax.fori_loop(0, S - 1 - me, hello, 0)
    pl.semaphore_signal(barrier, inc=1, device_id={"inner": mate}, device_id_type=MESH)

    loads = [
        pltpu.make_async_copy(src, dst, in_sem.at[i])
        for i, (src, dst) in enumerate(
            (
                (idx_hbm, slots.at[0]), (val_hbm, slots.at[1]),
                (k_ref, kv.at[0]), (v_ref, kv.at[1]), (q_ref, qd.at[0]), (do_ref, qd.at[1]),
            )
        )
    ]
    for load in loads:
        load.start()

    pl.semaphore_wait(barrier, me + 1)

    def answer(j, _):
        pl.semaphore_signal(ready.at[me], inc=1, device_id={"seq": j}, device_id_type=MESH)
        return 0

    lax.fori_loop(0, me, answer, 0)

    loads[0].wait()
    loads[1].wait()
    picked = jnp.where(slots[1] > 0, slots[0], -1)
    block = iota((lanes, total), 0)
    hit = jnp.zeros((lanes, total), F32)
    for t in range(topk):
        hit = jnp.where(picked[t : t + 1, :] == block, 1.0, hit)
    eye = jnp.where(iota((total, total), 0) == iota((total, total), 1), 1.0, 0.0).astype(BF)
    sel[...] = dot_nt(eye, hit.astype(BF))
    nb_shift = log2(nb)
    tri_r = iota((lanes, lanes), 0)
    tri_c = iota((lanes, lanes), 1)
    tri = jnp.where(
        (tri_r < tri_c)
        & (lax.shift_right_logical(tri_r, nb_shift) == lax.shift_right_logical(tri_c, nb_shift)),
        1.0,
        0.0,
    ).astype(BF)

    def ranks(run):
        rows = sel[pl.ds(pl.multiple_of(run * nb, nb), nb), :]
        present = jnp.max(rows, axis=0, keepdims=True)
        rank = dot(jnp.broadcast_to(present, (8, lanes)).astype(BF), tri)[0:1, :]
        return rows, present, rank

    def expand(axis):
        shape = (lanes, own_rows) if axis else (own_rows, lanes)
        block = lax.shift_right_logical(iota(shape, axis), log2(BLK)) + me * nb
        return jnp.where(block == iota(shape, 1 - axis), 1.0, 0.0).astype(BF)

    spread = expand(1)
    spread_t = expand(0)

    def send_a(r):
        return pltpu.make_async_remote_copy(
            src_ref=stage.at[r],
            dst_ref=pool.at[mate, pl.ds(pl.multiple_of(me * chunk, chunk), chunk)],
            send_sem=a_send.at[r],
            recv_sem=a_recv.at[me],
            device_id={"seq": r},
            device_id_type=MESH,
        )

    def code_of(r):
        _, present, rank = ranks(r)
        return jnp.broadcast_to(jnp.where(present > 0.5, rank, -8.0), (8, lanes)).astype(BF)

    def scatter_of(code):
        down = dot_nt(spread_t, jnp.broadcast_to(code[0:1, :], (chunk, lanes)))
        down = down.astype(jnp.int32) * BLK + (iota((own_rows, chunk), 0) & (BLK - 1))
        return jnp.where(down == iota((own_rows, chunk), 1), 1.0, 0.0).astype(BF)

    loads[2].wait()
    loads[3].wait()

    def choose(j, _):
        r = me + 1 + j
        code = code_of(r)
        across = dot(code, spread)[0:1, :].astype(jnp.int32) * BLK
        across = across + (iota((1, own_rows), 1) & (BLK - 1))
        pick = jnp.where(across == iota((chunk, own_rows), 0), 1.0, 0.0).astype(BF)
        stage[r] = dot(pick, kv[mate]).astype(BF)
        return 0

    lax.fori_loop(0, S - 1 - me, choose, 0)

    def give(j, _):
        r = me + 1 + j
        pl.semaphore_wait(ready.at[r], 1)
        send_a(r).start()
        return 0

    lax.fori_loop(0, S - 1 - me, give, 0)

    mine, present, rank = ranks(me)
    block_row = iota((1, lanes), 1)
    run_row = lax.shift_right_logical(block_row, nb_shift)
    place = jnp.where(
        run_row < me,
        run_row * CAP + rank.astype(jnp.int32),
        (S - 1) * CAP + (block_row & (nb - 1)),
    )
    place = jnp.where((present > 0.5) & (run_row <= me), place, -1)
    table = jnp.where(place == iota((slot_lanes, lanes), 0), 1.0, 0.0).astype(BF)
    bias = jnp.where(dot_nt(mine.astype(BF), table) > 0.5, 0.0, NEG)
    loads[4].wait()
    loads[5].wait()
    for b in range(nb):
        rows = pl.ds(b * rows_b, rows_b)
        qaug[rows, 0:width] = qd[0, rows, :]
        qaug[rows, width:] = jnp.broadcast_to(bias[b : b + 1, :], (rows_b, slot_lanes)).astype(BF)
    nkeys = oh.shape[0]
    oh[...] = jnp.where(
        lax.shift_right_logical(iota((nkeys, slot_lanes), 0), log2(BLK))
        == iota((nkeys, slot_lanes), 1),
        1.0,
        0.0,
    ).astype(BF)
    kt[:, nrem:] = kv[0].astype(F32).T.astype(BF)

    pair = 2 if nb % 2 == 0 else 1

    def own_count(b):
        return (b // pair + 1) * pair * BLK

    def fold(x, how):
        return how(how(x.reshape(-1, 8, rows_b), axis=0), axis=0, keepdims=True)

    def block_rows(b):
        return pl.ds(b * rows_b, rows_b)

    def soft(b, n, slot, keys_at):
        s = s_buf[b, 0:n, :]
        m = fold(s, jnp.max)
        e = jnp.exp2((s - m) * c2)
        st_m[slot, b : b + 1, :] = m
        st_l[slot, b : b + 1, :] = fold(e, jnp.sum)
        pd[1, keys_at, block_rows(b)] = e.astype(BF)

    def lean(b, slot, turned_v, keys_at):
        out = dot(turned_v, pd[1, keys_at, block_rows(b)])
        st_d[slot, b : b + 1, :] = fold(out * dot_t[:, block_rows(b)], jnp.sum)

    def grads(b, n, slot, vals, keys_at, delta):
        rows = block_rows(b)
        p = pd[1, keys_at, rows].astype(F32) * st_l[slot, b : b + 1, :]
        dp = dot_nt(vals, qd[1, rows, :])
        pd[1, keys_at, rows] = p.astype(BF)
        pd[0, keys_at, rows] = (p * (dp - delta[b : b + 1, :])).astype(BF)

    own_slot = S - 1
    st_m[...] = jnp.full((S, nb, rows_b), NEG, F32)
    st_l[...] = jnp.zeros((S, nb, rows_b), F32)
    st_d[...] = jnp.zeros((S, nb, rows_b), F32)
    vt_own[...] = kv[1].astype(F32).T.astype(BF)

    def own_scores(b):
        n = own_count(b)
        ka = jnp.concatenate([kv[0, 0:n, :], oh[nrem : nrem + n, :]], axis=1)
        s = dot_nt(ka, qaug[block_rows(b), :])
        lo, hi = b * BLK, (b + 1) * BLK
        if lo:
            s_buf[b, 0:lo, :] = s[0:lo]
        key = iota((BLK, rows_b), 0)
        query = lax.shift_right_logical(iota((BLK, rows_b), 1), log2(heads))
        s_buf[b, lo:hi, :] = jnp.where(key > query, NEG, s[lo:hi])
        if hi < n:
            s_buf[b, hi:n, :] = s[hi:n]

    def ahead(first, then):
        first(0)
        for b in range(nb):
            if b + 1 < nb:
                first(b + 1)
            then(b)

    ahead(own_scores, lambda b: soft(b, own_count(b), own_slot, pl.ds(nrem, own_count(b))))
    for b in range(nb):
        rows = block_rows(b)
        dot_t[:, rows] = qd[1, rows, :].astype(F32).T
        n = own_count(b)
        lean(b, own_slot, vt_own[:, 0:n], pl.ds(nrem, n))

    if pre:

        def scatters(j, _):
            r = me + 1 + j
            wt[r] = scatter_of(code_of(r))
            return 0

        lax.fori_loop(0, S - 1 - me, scatters, 0)

    def blank(s, _):
        at = pl.ds(pl.multiple_of(s * chunk, chunk), chunk)
        pool[0, at, :] = jnp.zeros((chunk, width), BF)
        pool[1, at, :] = jnp.zeros((chunk, width), BF)
        for b in range(nb):
            pd[0, at, block_rows(b)] = jnp.zeros((chunk, rows_b), BF)
        return 0

    lax.fori_loop(me, S - 1, blank, 0)

    def pool_at(kind, s):
        return pool.at[kind, pl.ds(pl.multiple_of(s * chunk, chunk), chunk)]

    def recv_a(s):
        return pltpu.make_async_remote_copy(
            src_ref=stage.at[s],
            dst_ref=pool_at(mate, s),
            send_sem=a_send.at[s],
            recv_sem=a_recv.at[s],
            device_id={"seq": s},
            device_id_type=MESH,
        )

    def forward(kind, s):
        return pltpu.make_async_remote_copy(
            src_ref=pool_at(kind, s),
            dst_ref=pool_at(kind, s),
            send_sem=f_send.at[s],
            recv_sem=f_recv.at[s],
            device_id={"inner": mate},
            device_id_type=MESH,
        )

    def keys_of(s):
        return pl.ds(pl.multiple_of(s * chunk, chunk), chunk)

    def partial(s):
        at = keys_of(s)
        vt[s] = pool[1, at, :].astype(F32).T.astype(BF)

        def scores(b):
            ka = jnp.concatenate([pool[0, at, :], oh[at, :]], axis=1)
            s_buf[b, 0:chunk, :] = dot_nt(ka, qaug[block_rows(b), :])

        ahead(scores, lambda b: soft(b, chunk, s, at))
        for b in range(nb):
            lean(b, s, vt[s], at)

    def arrive(j, _):
        @pl.when(j < me)
        def _():
            s = me - 1 - j
            recv_a(s).wait_recv()
            forward(mate, s).start()

        @pl.when(j > 0)
        def _():
            s = me - j
            forward(core, s).wait_recv()
            partial(s)

        return 0

    lax.fori_loop(0, me + 1, arrive, 0)

    top = st_m[0]
    for s in range(1, S):
        top = jnp.maximum(top, st_m[s])
    mass = jnp.zeros((nb, rows_b), F32)
    delta = jnp.zeros((nb, rows_b), F32)
    for s in range(S):
        w = jnp.exp2((st_m[s] - top) * c2)
        st_m[s] = w
        mass += w * st_l[s]
        delta += w * st_d[s]
    inv = 1.0 / mass
    st_d[0] = delta * inv
    for s in range(S):
        st_l[s] = st_m[s] * inv

    def scale_of(kind):
        return jnp.where(kind == 0, scaling, 1.0).astype(F32)

    def swap(s):
        return pltpu.make_async_remote_copy(
            src_ref=terms.at[s, mate],
            dst_ref=xrecv.at[s],
            send_sem=x_send.at[s],
            recv_sem=x_recv.at[s],
            device_id={"inner": mate},
            device_id_type=MESH,
        )

    def give_back(s):
        return pltpu.make_async_remote_copy(
            src_ref=tsend.at[s],
            dst_ref=trecv.at[me],
            send_sem=t_send.at[s],
            recv_sem=t_recv.at[me],
            device_id={"seq": s},
            device_id_type=MESH,
        )

    def finish(s):
        swap(s).wait_recv()
        tsend[s] = (terms[s, core] + xrecv[s]).astype(BF)
        give_back(s).start()

    def remote(s, _):
        at = keys_of(s)
        delta = st_d[0]
        for b in range(nb):
            grads(b, chunk, s, pool[1, at, :], at, delta)
        terms[s, 1] = dot(pd[1, at, :], qd[1])
        terms[s, 0] = dot(pd[0, at, :], qd[0]) * scaling
        swap(s).start()

        @pl.when(s > 0)
        def _():
            finish(s - 1)

        return 0

    lax.fori_loop(0, me, remote, 0)

    @pl.when(me > 0)
    def _():
        finish(me - 1)

    own_swap = pltpu.make_async_remote_copy(
        src_ref=ox_send,
        dst_ref=ox_recv,
        send_sem=o_sem.at[0],
        recv_sem=o_sem.at[1],
        device_id={"inner": mate},
        device_id_type=MESH,
    )

    def own_terms(kind, target):
        for c in range(0, nb, pair):
            n = pair * BLK
            lo = c * rows_b
            target[c * BLK : c * BLK + n, :] = (
                dot(pd[kind, nrem + c * BLK : nrem + c * BLK + n, lo:], qd[kind, lo:, :])
                * scale_of(kind)
            )

    delta = st_d[0]
    for b in range(nb):
        n = own_count(b)
        grads(b, n, own_slot, kv[1, 0:n, :], pl.ds(nrem, n), delta)
    own_terms(mate, ox_send)
    own_swap.start()
    own_terms(core, acc)

    for s in range(S - 1):
        kt[:, s * chunk : (s + 1) * chunk] = (
            pool[0, s * chunk : (s + 1) * chunk, :].astype(F32).T.astype(BF)
        )
    for b in range(nb):
        rows = pl.ds(b * rows_b, rows_b)
        n = nrem + own_count(b)
        turned = dot(kt[:, 0:n], pd[0, 0:n, rows]) * scaling
        dq_ref[rows, :] = turned.T.astype(BF)

    own_swap.wait_recv()
    acc[...] += ox_recv[...]

    def gather(j, _):
        r = me + 1 + j
        pltpu.make_async_remote_copy(
            src_ref=tsend.at[r],
            dst_ref=trecv.at[r],
            send_sem=t_send.at[r],
            recv_sem=t_recv.at[r],
            device_id={"seq": r},
            device_id_type=MESH,
        ).wait_recv()
        acc[...] += dot(wt[r] if pre else scatter_of(code_of(r)), trecv[r])
        return 0

    lax.fori_loop(0, S - 1 - me, gather, 0)

    def last(ref):
        return pltpu.make_async_remote_copy(
            src_ref=ref,
            dst_ref=ref,
            send_sem=r_sem.at[0],
            recv_sem=r_sem.at[1],
            device_id={"inner": mate},
            device_id_type=MESH,
        )

    @pl.when(core == 0)
    def _():
        dk_ref[...] = acc[...].astype(BF)
        last(dk_ref).start()

    @pl.when(core == 1)
    def _():
        dv_ref[...] = acc[...].astype(BF)
        last(dv_ref).start()

    def close_up(j, _):
        send_a(me + 1 + j).wait_send()
        return 0

    lax.fori_loop(0, S - 1 - me, close_up, 0)

    def close_down(s, _):
        forward(mate, s).wait_send()
        swap(s).wait_send()
        give_back(s).wait_send()
        return 0

    lax.fori_loop(0, me, close_down, 0)
    own_swap.wait_send()

    @pl.when(core == 0)
    def _():
        last(dk_ref).wait_send()
        last(dv_ref).wait_recv()

    @pl.when(core == 1)
    def _():
        last(dv_ref).wait_send()
        last(dk_ref).wait_recv()


def place_kernel(*refs):
    n = len(refs) // 2
    moves = [pltpu.make_async_copy(refs[i], refs[n + i], refs[-1].at[i]) for i in range(n)]
    for move in moves:
        move.start()
    for move in moves:
        move.wait()


def place(*arrays):
    return pl.pallas_call(
        place_kernel,
        out_shape=tuple(jax.ShapeDtypeStruct(a.shape, a.dtype) for a in arrays),
        in_specs=[pl.BlockSpec(memory_space=pltpu.VMEM)] * len(arrays),
        out_specs=(pl.BlockSpec(memory_space=pl.ANY),) * len(arrays),
        scratch_shapes=[pltpu.SemaphoreType.DMA((len(arrays),))],
        compiler_params=pltpu.CompilerParams(vmem_limit_bytes=65536),
    )(*(pltpu.with_memory_space_constraint(a, pltpu.VMEM) for a in arrays))


def per_device(queries, grad_out, keys, values, indices, valid):
    tokens, _, heads, width = queries.shape
    S = lax.axis_size("seq")
    total, topk = indices.shape[1:]
    nb = tokens // BLK
    chunk = CAP * BLK
    nrem = (S - 1) * chunk
    own_rows = tokens
    nkeys = nrem + own_rows
    rows = tokens * heads
    rows_b = BLK * heads
    lanes = -(-total // 128) * 128
    slot_lanes = -(-(nkeys // BLK) // 128) * 128
    pre = S <= 4
    cfg = (S, heads, nb, total, topk, width, pre)
    vmem = pl.BlockSpec(memory_space=pltpu.VMEM)
    hbm = pl.BlockSpec(memory_space=pl.ANY)
    dma = pltpu.SemaphoreType.DMA
    dq, dk, dv = pl.pallas_call(
        functools.partial(kernel, cfg),
        out_shape=(
            pltpu.VMEM((rows, width), BF),
            pltpu.VMEM((own_rows, width), BF),
            pltpu.VMEM((own_rows, width), BF),
        ),
        in_specs=[hbm] * 6,
        out_specs=(vmem, vmem, vmem),
        scratch_shapes=[
            pltpu.VMEM((total, lanes), F32),
            pltpu.VMEM((rows, width + slot_lanes), BF),
            pltpu.VMEM((2, rows, width), BF),
            pltpu.VMEM((2, own_rows, width), BF),
            pltpu.VMEM((nkeys, slot_lanes), BF),
            pltpu.VMEM((width, nkeys), BF),
            pltpu.VMEM((S - 1, width, chunk), BF),
            pltpu.VMEM((width, own_rows), BF),
            pltpu.VMEM((width, rows), F32),
            pltpu.VMEM((S, chunk, width), BF),
            pltpu.VMEM((2, nrem, width), BF),
            pltpu.VMEM((S if pre else 1, own_rows, chunk), BF),
            pltpu.VMEM((nb, max(own_rows, chunk), rows_b), F32),
            pltpu.VMEM((2, nkeys, rows), BF),
            pltpu.VMEM((S, 2, chunk, width), F32),
            pltpu.VMEM((S, chunk, width), F32),
            pltpu.VMEM((S, chunk, width), BF),
            pltpu.VMEM((S, chunk, width), BF),
            pltpu.VMEM((own_rows, width), F32),
            pltpu.VMEM((own_rows, width), F32),
            pltpu.VMEM((own_rows, width), F32),
            dma((S,)), dma((S,)), dma((S,)), dma((S,)), dma((S,)), dma((S,)),
            dma((S,)), dma((S,)), dma((2,)), dma((2,)),
            dma((6,)),
            pltpu.SemaphoreType.REGULAR((S,)),
            pltpu.VMEM((2, topk, total), jnp.int32),
            pltpu.VMEM((S, nb, rows_b), F32),
            pltpu.VMEM((S, nb, rows_b), F32),
            pltpu.VMEM((S, nb, rows_b), F32),
        ],
        compiler_params=pltpu.CompilerParams(
            collective_id=0, has_side_effects=True, vmem_limit_bytes=67043328 - 6 * own_rows * width * 2 - 4096
        ),
    )(
        queries.reshape(rows, width),
        grad_out.reshape(rows, width),
        keys.reshape(own_rows, width),
        values.reshape(own_rows, width),
        indices[0].T,
        valid[0].T,
    )
    dq, dk, dv = place(dq, dk, dv)
    return (
        dq.reshape(tokens, 1, heads, width),
        dk.reshape(tokens, 1, width),
        dv.reshape(tokens, 1, width),
    )


def solution(mesh):
    return jax.shard_map(
        per_device,
        mesh=mesh,
        in_specs=(
            P(("groups", "seq"), "head", "inner", None),
            P(("groups", "seq"), "head", "inner", None),
            P(("groups", "seq"), "head", None),
            P(("groups", "seq"), "head", None),
            P("head", "groups", None),
            P("head", "groups", None),
        ),
        out_specs=(
            P(("groups", "seq"), "head", "inner", None),
            P(("groups", "seq"), "head", None),
            P(("groups", "seq"), "head", None),
        ),
        check_vma=False,
    )
```

```python
import functools
import math

import jax
import jax.numpy as jnp
from jax import lax
from jax.experimental import pallas as pl
from jax.experimental.pallas import tpu as pltpu
from jax.sharding import PartitionSpec as P

BLK = 64
CAP = 4
MESH = pl.DeviceIdType.MESH
NEG = -1e30
NT = (((1,), (1,)), ((), ()))
F32 = jnp.float32
BF = jnp.bfloat16


def dot(a, b):
    return jnp.dot(a, b, preferred_element_type=F32)


def dot_nt(a, b):
    return lax.dot_general(a, b, NT, preferred_element_type=F32)


def log2(n):
    shift = n.bit_length() - 1
    assert 1 << shift == n
    return shift


def iota(shape, axis):
    return lax.broadcasted_iota(jnp.int32, shape, axis)


def kernel(
    cfg,
    q_ref, do_ref, k_ref, v_ref, idx_hbm, val_hbm,
    dq_ref, dk_ref, dv_ref,
    sel, qaug, qd, kv, oh, kt, vt_own, dot_t, stage, pool, wt,
    s_buf, pd, terms, xrecv, tsend, trecv, ox_send, ox_recv, acc,
    a_send, a_recv, f_send, f_recv, x_send, x_recv, t_send, t_recv, o_sem, r_sem, in_sem,
    ready, slots, st_m, st_l, st_d,
):
    S, heads, nb, total, topk, width, pre = cfg
    me = lax.axis_index("seq")
    core = lax.axis_index("inner")
    mate = 1 - core
    chunk = CAP * BLK
    nrem = (S - 1) * chunk
    rows_b = BLK * heads
    own_rows = nb * BLK
    lanes = sel.shape[1]
    slot_lanes = oh.shape[1]
    scaling = 1.0 / math.sqrt(width)
    c2 = scaling * math.log2(math.e)

    barrier = pltpu.get_barrier_semaphore()

    def hello(j, _):
        pl.semaphore_signal(barrier, inc=1, device_id={"seq": S - 1 - j}, device_id_type=MESH)
        return 0

    lax.fori_loop(0, S - 1 - me, hello, 0)
    pl.semaphore_signal(barrier, inc=1, device_id={"inner": mate}, device_id_type=MESH)

    loads = [
        pltpu.make_async_copy(src, dst, in_sem.at[i])
        for i, (src, dst) in enumerate(
            (
                (idx_hbm, slots.at[0]), (val_hbm, slots.at[1]),
                (k_ref, kv.at[0]), (v_ref, kv.at[1]), (q_ref, qd.at[0]), (do_ref, qd.at[1]),
            )
        )
    ]
    for load in loads:
        load.start()

    pl.semaphore_wait(barrier, me + 1)

    def answer(j, _):
        pl.semaphore_signal(ready.at[me], inc=1, device_id={"seq": j}, device_id_type=MESH)
        return 0

    lax.fori_loop(0, me, answer, 0)

    loads[0].wait()
    loads[1].wait()
    picked = jnp.where(slots[1] > 0, slots[0], -1)
    block = iota((lanes, total), 0)
    hit = jnp.zeros((lanes, total), F32)
    for t in range(topk):
        hit = jnp.where(picked[t : t + 1, :] == block, 1.0, hit)
    eye = jnp.where(iota((total, total), 0) == iota((total, total), 1), 1.0, 0.0).astype(BF)
    sel[...] = dot_nt(eye, hit.astype(BF))
    nb_shift = log2(nb)
    tri_r = iota((lanes, lanes), 0)
    tri_c = iota((lanes, lanes), 1)
    tri = jnp.where(
        (tri_r < tri_c)
        & (lax.shift_right_logical(tri_r, nb_shift) == lax.shift_right_logical(tri_c, nb_shift)),
        1.0,
        0.0,
    ).astype(BF)

    def ranks(run):
        rows = sel[pl.ds(pl.multiple_of(run * nb, nb), nb), :]
        present = jnp.max(rows, axis=0, keepdims=True)
        rank = dot(jnp.broadcast_to(present, (8, lanes)).astype(BF), tri)[0:1, :]
        return rows, present, rank

    def expand(axis):
        shape = (lanes, own_rows) if axis else (own_rows, lanes)
        block = lax.shift_right_logical(iota(shape, axis), log2(BLK)) + me * nb
        return jnp.where(block == iota(shape, 1 - axis), 1.0, 0.0).astype(BF)

    spread = expand(1)
    spread_t = expand(0)

    def send_a(r):
        return pltpu.make_async_remote_copy(
            src_ref=stage.at[r],
            dst_ref=pool.at[mate, pl.ds(pl.multiple_of(me * chunk, chunk), chunk)],
            send_sem=a_send.at[r],
            recv_sem=a_recv.at[me],
            device_id={"seq": r},
            device_id_type=MESH,
        )

    def code_of(r):
        _, present, rank = ranks(r)
        return jnp.broadcast_to(jnp.where(present > 0.5, rank, -8.0), (8, lanes)).astype(BF)

    def scatter_of(code):
        down = dot_nt(spread_t, jnp.broadcast_to(code[0:1, :], (chunk, lanes)))
        down = down.astype(jnp.int32) * BLK + (iota((own_rows, chunk), 0) & (BLK - 1))
        return jnp.where(down == iota((own_rows, chunk), 1), 1.0, 0.0).astype(BF)

    loads[2].wait()
    loads[3].wait()

    def choose(j, _):
        r = me + 1 + j
        code = code_of(r)
        across = dot(code, spread)[0:1, :].astype(jnp.int32) * BLK
        across = across + (iota((1, own_rows), 1) & (BLK - 1))
        pick = jnp.where(across == iota((chunk, own_rows), 0), 1.0, 0.0).astype(BF)
        stage[r] = dot(pick, kv[mate]).astype(BF)
        return 0

    lax.fori_loop(0, S - 1 - me, choose, 0)

    def give(j, _):
        r = me + 1 + j
        pl.semaphore_wait(ready.at[r], 1)
        send_a(r).start()
        return 0

    lax.fori_loop(0, S - 1 - me, give, 0)

    mine, present, rank = ranks(me)
    block_row = iota((1, lanes), 1)
    run_row = lax.shift_right_logical(block_row, nb_shift)
    place = jnp.where(
        run_row < me,
        run_row * CAP + rank.astype(jnp.int32),
        (S - 1) * CAP + (block_row & (nb - 1)),
    )
    place = jnp.where((present > 0.5) & (run_row <= me), place, -1)
    table = jnp.where(place == iota((slot_lanes, lanes), 0), 1.0, 0.0).astype(BF)
    bias = jnp.where(dot_nt(mine.astype(BF), table) > 0.5, 0.0, NEG)
    loads[4].wait()
    loads[5].wait()
    for b in range(nb):
        rows = pl.ds(b * rows_b, rows_b)
        qaug[rows, 0:width] = qd[0, rows, :]
        qaug[rows, width:] = jnp.broadcast_to(bias[b : b + 1, :], (rows_b, slot_lanes)).astype(BF)
    nkeys = oh.shape[0]
    oh[...] = jnp.where(
        lax.shift_right_logical(iota((nkeys, slot_lanes), 0), log2(BLK))
        == iota((nkeys, slot_lanes), 1),
        1.0,
        0.0,
    ).astype(BF)
    kt[:, nrem:] = kv[0].astype(F32).T.astype(BF)

    pair = 2 if nb % 2 == 0 else 1

    def own_count(b):
        return (b // pair + 1) * pair * BLK

    def fold(x, how):
        return how(how(x.reshape(-1, 8, rows_b), axis=0), axis=0, keepdims=True)

    def block_rows(b):
        return pl.ds(b * rows_b, rows_b)

    def soft(b, n, slot, keys_at):
        e = jnp.exp2((s_buf[b, 0:n, :] - st_m[slot, b : b + 1, :]) * c2)
        st_l[slot, b : b + 1, :] = fold(e, jnp.sum)
        pd[1, keys_at, block_rows(b)] = e.astype(BF)

    def lean(b, slot, turned_v, keys_at):
        out = dot(turned_v, pd[1, keys_at, block_rows(b)])
        st_d[slot, b : b + 1, :] = fold(out * dot_t[:, block_rows(b)], jnp.sum)

    def grads(b, n, slot, vals, keys_at, delta):
        rows = block_rows(b)
        p = pd[1, keys_at, rows].astype(F32) * st_l[slot, b : b + 1, :]
        dp = dot_nt(vals, qd[1, rows, :])
        pd[1, keys_at, rows] = p.astype(BF)
        pd[0, keys_at, rows] = (p * (dp - delta[b : b + 1, :])).astype(BF)

    own_slot = S - 1
    st_m[...] = jnp.full((S, nb, rows_b), NEG, F32)
    st_l[...] = jnp.zeros((S, nb, rows_b), F32)
    st_d[...] = jnp.zeros((S, nb, rows_b), F32)
    vt_own[...] = kv[1].astype(F32).T.astype(BF)

    def own_scores(b):
        n = own_count(b)
        ka = jnp.concatenate([kv[0, 0:n, :], oh[nrem : nrem + n, :]], axis=1)
        s = dot_nt(ka, qaug[block_rows(b), :])
        lo, hi = b * BLK, (b + 1) * BLK
        key = iota((BLK, rows_b), 0)
        query = lax.shift_right_logical(iota((BLK, rows_b), 1), log2(heads))
        parts = [jnp.where(key > query, NEG, s[lo:hi])]
        if lo:
            parts.insert(0, s[0:lo])
        if hi < n:
            parts.append(s[hi:n])
        s = jnp.concatenate(parts, axis=0)
        s_buf[b, 0:n, :] = s
        st_m[own_slot, b : b + 1, :] = fold(s, jnp.max)

    def ahead(first, then):
        first(0)
        for b in range(nb):
            if b + 1 < nb:
                first(b + 1)
            then(b)

    ahead(own_scores, lambda b: soft(b, own_count(b), own_slot, pl.ds(nrem, own_count(b))))
    for b in range(nb):
        rows = block_rows(b)
        dot_t[:, rows] = qd[1, rows, :].astype(F32).T
        n = own_count(b)
        lean(b, own_slot, vt_own[:, 0:n], pl.ds(nrem, n))

    if pre:

        def scatters(j, _):
            r = me + 1 + j
            wt[r] = scatter_of(code_of(r))
            return 0

        lax.fori_loop(0, S - 1 - me, scatters, 0)

    def blank(s, _):
        at = pl.ds(pl.multiple_of(s * chunk, chunk), chunk)
        pool[0, at, :] = jnp.zeros((chunk, width), BF)
        pool[1, at, :] = jnp.zeros((chunk, width), BF)
        for b in range(nb):
            pd[0, at, block_rows(b)] = jnp.zeros((chunk, rows_b), BF)
        return 0

    lax.fori_loop(me, S - 1, blank, 0)

    def pool_at(kind, s):
        return pool.at[kind, pl.ds(pl.multiple_of(s * chunk, chunk), chunk)]

    def recv_a(s):
        return pltpu.make_async_remote_copy(
            src_ref=stage.at[s],
            dst_ref=pool_at(mate, s),
            send_sem=a_send.at[s],
            recv_sem=a_recv.at[s],
            device_id={"seq": s},
            device_id_type=MESH,
        )

    def forward(kind, s):
        return pltpu.make_async_remote_copy(
            src_ref=pool_at(kind, s),
            dst_ref=pool_at(kind, s),
            send_sem=f_send.at[s],
            recv_sem=f_recv.at[s],
            device_id={"inner": mate},
            device_id_type=MESH,
        )

    def keys_of(s):
        return pl.ds(pl.multiple_of(s * chunk, chunk), chunk)

    def weigh(s):
        at = keys_of(s)

        def scores(b):
            ka = jnp.concatenate([pool[0, at, :], oh[at, :]], axis=1)
            part = dot_nt(ka, qaug[block_rows(b), :])
            s_buf[b, 0:chunk, :] = part
            st_m[s, b : b + 1, :] = fold(part, jnp.max)

        ahead(scores, lambda b: soft(b, chunk, s, at))

    def average(s):
        at = keys_of(s)
        turned_v = pool[1, at, :].astype(F32).T.astype(BF)
        for b in range(nb):
            lean(b, s, turned_v, at)

    def land(s):
        recv_a(s).wait_recv()
        forward(mate, s).start()

    def keys_in(s):
        @pl.when(core == 1)
        def _():
            land(s)

        @pl.when(core == 0)
        def _():
            forward(core, s).wait_recv()

        weigh(s)

    def values_in(s):
        @pl.when(core == 1)
        def _():
            forward(core, s).wait_recv()

        average(s)

    def down(first, body):
        def at(j, _):
            body(me - 1 - j)
            return 0

        lax.fori_loop(first, me, at, 0)

    @pl.when(me > 0)
    def _():
        keys_in(me - 1)

    @pl.when(core == 0)
    def _():
        down(0, land)

    down(1, keys_in)
    down(0, values_in)

    top = st_m[0]
    for s in range(1, S):
        top = jnp.maximum(top, st_m[s])
    mass = jnp.zeros((nb, rows_b), F32)
    delta = jnp.zeros((nb, rows_b), F32)
    for s in range(S):
        w = jnp.exp2((st_m[s] - top) * c2)
        st_m[s] = w
        mass += w * st_l[s]
        delta += w * st_d[s]
    inv = 1.0 / mass
    st_d[0] = delta * inv
    for s in range(S):
        st_l[s] = st_m[s] * inv

    def scale_of(kind):
        return jnp.where(kind == 0, scaling, 1.0).astype(F32)

    def swap(s):
        return pltpu.make_async_remote_copy(
            src_ref=terms.at[s, mate],
            dst_ref=xrecv.at[s],
            send_sem=x_send.at[s],
            recv_sem=x_recv.at[s],
            device_id={"inner": mate},
            device_id_type=MESH,
        )

    def give_back(s):
        return pltpu.make_async_remote_copy(
            src_ref=tsend.at[s],
            dst_ref=trecv.at[me],
            send_sem=t_send.at[s],
            recv_sem=t_recv.at[me],
            device_id={"seq": s},
            device_id_type=MESH,
        )

    def finish(s):
        swap(s).wait_recv()
        tsend[s] = (terms[s, core] + xrecv[s]).astype(BF)
        give_back(s).start()

    def remote(s, _):
        at = keys_of(s)
        delta = st_d[0]
        for b in range(nb):
            grads(b, chunk, s, pool[1, at, :], at, delta)
        terms[s, 1] = dot(pd[1, at, :], qd[1])
        terms[s, 0] = dot(pd[0, at, :], qd[0]) * scaling
        swap(s).start()

        @pl.when(s > 0)
        def _():
            finish(s - 1)

        return 0

    lax.fori_loop(0, me, remote, 0)

    @pl.when(me > 0)
    def _():
        finish(me - 1)

    own_swap = pltpu.make_async_remote_copy(
        src_ref=ox_send,
        dst_ref=ox_recv,
        send_sem=o_sem.at[0],
        recv_sem=o_sem.at[1],
        device_id={"inner": mate},
        device_id_type=MESH,
    )

    def own_terms(kind, target):
        for c in range(0, nb, pair):
            n = pair * BLK
            lo = c * rows_b
            target[c * BLK : c * BLK + n, :] = (
                dot(pd[kind, nrem + c * BLK : nrem + c * BLK + n, lo:], qd[kind, lo:, :])
                * scale_of(kind)
            )

    delta = st_d[0]
    for b in range(nb):
        n = own_count(b)
        grads(b, n, own_slot, kv[1, 0:n, :], pl.ds(nrem, n), delta)
    own_terms(mate, ox_send)
    own_swap.start()
    own_terms(core, acc)

    for s in range(S - 1):
        kt[:, s * chunk : (s + 1) * chunk] = (
            pool[0, s * chunk : (s + 1) * chunk, :].astype(F32).T.astype(BF)
        )
    for b in range(nb):
        rows = pl.ds(b * rows_b, rows_b)
        n = nrem + own_count(b)
        turned = dot(kt[:, 0:n], pd[0, 0:n, rows]) * scaling
        dq_ref[rows, :] = turned.T.astype(BF)

    own_swap.wait_recv()
    acc[...] += ox_recv[...]

    def gather(j, _):
        r = me + 1 + j
        pltpu.make_async_remote_copy(
            src_ref=tsend.at[r],
            dst_ref=trecv.at[r],
            send_sem=t_send.at[r],
            recv_sem=t_recv.at[r],
            device_id={"seq": r},
            device_id_type=MESH,
        ).wait_recv()
        acc[...] += dot(wt[r] if pre else scatter_of(code_of(r)), trecv[r])
        return 0

    lax.fori_loop(0, S - 1 - me, gather, 0)

    def last(ref):
        return pltpu.make_async_remote_copy(
            src_ref=ref,
            dst_ref=ref,
            send_sem=r_sem.at[0],
            recv_sem=r_sem.at[1],
            device_id={"inner": mate},
            device_id_type=MESH,
        )

    @pl.when(core == 0)
    def _():
        dk_ref[...] = acc[...].astype(BF)
        last(dk_ref).start()

    @pl.when(core == 1)
    def _():
        dv_ref[...] = acc[...].astype(BF)
        last(dv_ref).start()

    def close_up(j, _):
        send_a(me + 1 + j).wait_send()
        return 0

    lax.fori_loop(0, S - 1 - me, close_up, 0)

    def close_down(s, _):
        forward(mate, s).wait_send()
        swap(s).wait_send()
        give_back(s).wait_send()
        return 0

    lax.fori_loop(0, me, close_down, 0)
    own_swap.wait_send()

    @pl.when(core == 0)
    def _():
        last(dk_ref).wait_send()
        last(dv_ref).wait_recv()

    @pl.when(core == 1)
    def _():
        last(dv_ref).wait_send()
        last(dk_ref).wait_recv()


def place_kernel(*refs):
    n = len(refs) // 2
    moves = [pltpu.make_async_copy(refs[i], refs[n + i], refs[-1].at[i]) for i in range(n)]
    for move in moves:
        move.start()
    for move in moves:
        move.wait()


def place(*arrays):
    return pl.pallas_call(
        place_kernel,
        out_shape=tuple(jax.ShapeDtypeStruct(a.shape, a.dtype) for a in arrays),
        in_specs=[pl.BlockSpec(memory_space=pltpu.VMEM)] * len(arrays),
        out_specs=(pl.BlockSpec(memory_space=pl.ANY),) * len(arrays),
        scratch_shapes=[pltpu.SemaphoreType.DMA((len(arrays),))],
        compiler_params=pltpu.CompilerParams(vmem_limit_bytes=65536),
    )(*(pltpu.with_memory_space_constraint(a, pltpu.VMEM) for a in arrays))


def per_device(queries, grad_out, keys, values, indices, valid):
    tokens, _, heads, width = queries.shape
    S = lax.axis_size("seq")
    total, topk = indices.shape[1:]
    nb = tokens // BLK
    chunk = CAP * BLK
    nrem = (S - 1) * chunk
    own_rows = tokens
    nkeys = nrem + own_rows
    rows = tokens * heads
    rows_b = BLK * heads
    lanes = -(-total // 128) * 128
    slot_lanes = -(-(nkeys // BLK) // 128) * 128
    pre = S <= 4
    cfg = (S, heads, nb, total, topk, width, pre)
    vmem = pl.BlockSpec(memory_space=pltpu.VMEM)
    hbm = pl.BlockSpec(memory_space=pl.ANY)
    dma = pltpu.SemaphoreType.DMA
    dq, dk, dv = pl.pallas_call(
        functools.partial(kernel, cfg),
        out_shape=(
            pltpu.VMEM((rows, width), BF),
            pltpu.VMEM((own_rows, width), BF),
            pltpu.VMEM((own_rows, width), BF),
        ),
        in_specs=[hbm] * 6,
        out_specs=(vmem, vmem, vmem),
        scratch_shapes=[
            pltpu.VMEM((total, lanes), F32),
            pltpu.VMEM((rows, width + slot_lanes), BF),
            pltpu.VMEM((2, rows, width), BF),
            pltpu.VMEM((2, own_rows, width), BF),
            pltpu.VMEM((nkeys, slot_lanes), BF),
            pltpu.VMEM((width, nkeys), BF),
            pltpu.VMEM((width, own_rows), BF),
            pltpu.VMEM((width, rows), F32),
            pltpu.VMEM((S, chunk, width), BF),
            pltpu.VMEM((2, nrem, width), BF),
            pltpu.VMEM((S if pre else 1, own_rows, chunk), BF),
            pltpu.VMEM((nb, max(own_rows, chunk), rows_b), F32),
            pltpu.VMEM((2, nkeys, rows), BF),
            pltpu.VMEM((S, 2, chunk, width), F32),
            pltpu.VMEM((S, chunk, width), F32),
            pltpu.VMEM((S, chunk, width), BF),
            pltpu.VMEM((S, chunk, width), BF),
            pltpu.VMEM((own_rows, width), F32),
            pltpu.VMEM((own_rows, width), F32),
            pltpu.VMEM((own_rows, width), F32),
            dma((S,)), dma((S,)), dma((S,)), dma((S,)), dma((S,)), dma((S,)),
            dma((S,)), dma((S,)), dma((2,)), dma((2,)),
            dma((6,)),
            pltpu.SemaphoreType.REGULAR((S,)),
            pltpu.VMEM((2, topk, total), jnp.int32),
            pltpu.VMEM((S, nb, rows_b), F32),
            pltpu.VMEM((S, nb, rows_b), F32),
            pltpu.VMEM((S, nb, rows_b), F32),
        ],
        compiler_params=pltpu.CompilerParams(
            collective_id=0, has_side_effects=True, vmem_limit_bytes=67043328 - 6 * own_rows * width * 2 - 4096
        ),
    )(
        queries.reshape(rows, width),
        grad_out.reshape(rows, width),
        keys.reshape(own_rows, width),
        values.reshape(own_rows, width),
        indices[0].T,
        valid[0].T,
    )
    dq, dk, dv = place(dq, dk, dv)
    return (
        dq.reshape(tokens, 1, heads, width),
        dk.reshape(tokens, 1, width),
        dv.reshape(tokens, 1, width),
    )


def solution(mesh):
    return jax.shard_map(
        per_device,
        mesh=mesh,
        in_specs=(
            P(("groups", "seq"), "head", "inner", None),
            P(("groups", "seq"), "head", "inner", None),
            P(("groups", "seq"), "head", None),
            P(("groups", "seq"), "head", None),
            P("head", "groups", None),
            P("head", "groups", None),
        ),
        out_specs=(
            P(("groups", "seq"), "head", "inner", None),
            P(("groups", "seq"), "head", None),
            P(("groups", "seq"), "head", None),
        ),
        check_vma=False,
    )
```

```python
import functools
import math

import jax
import jax.numpy as jnp
from jax import lax
from jax.experimental import pallas as pl
from jax.experimental.pallas import tpu as pltpu
from jax.sharding import PartitionSpec as P

BLK = 64
CAP = 4
MESH = pl.DeviceIdType.MESH
NEG = -1e30
NT = (((1,), (1,)), ((), ()))
F32 = jnp.float32
BF = jnp.bfloat16


def dot(a, b):
    return jnp.dot(a, b, preferred_element_type=F32)


def dot_nt(a, b):
    return lax.dot_general(a, b, NT, preferred_element_type=F32)


def log2(n):
    shift = n.bit_length() - 1
    assert 1 << shift == n
    return shift


def iota(shape, axis):
    return lax.broadcasted_iota(jnp.int32, shape, axis)


def kernel(
    cfg,
    q_ref, do_ref, k_ref, v_ref, idx_hbm, val_hbm,
    dq_ref, dk_ref, dv_ref,
    sel, qaug, qd, kv, oh, kt, vt_own, dot_t, stage, pool, wt,
    s_buf, pd, p_run, terms, xrecv, tsend, trecv, ox_send, ox_recv, acc,
    a_send, a_recv, f_send, f_recv, x_send, x_recv, t_send, t_recv, o_sem, r_sem, in_sem,
    ready, slots, st_m, st_l, st_d,
):
    S, heads, nb, total, topk, width, pre = cfg
    me = lax.axis_index("seq")
    core = lax.axis_index("inner")
    mate = 1 - core
    chunk = CAP * BLK
    nrem = (S - 1) * chunk
    rows_b = BLK * heads
    own_rows = nb * BLK
    lanes = sel.shape[1]
    slot_lanes = oh.shape[1]
    scaling = 1.0 / math.sqrt(width)
    c2 = scaling * math.log2(math.e)

    barrier = pltpu.get_barrier_semaphore()

    def hello(j, _):
        pl.semaphore_signal(barrier, inc=1, device_id={"seq": S - 1 - j}, device_id_type=MESH)
        return 0

    lax.fori_loop(0, S - 1 - me, hello, 0)
    middle = S // 2

    @pl.when(me == middle)
    def _():
        pl.semaphore_signal(barrier, inc=1, device_id={"seq": middle - 1}, device_id_type=MESH)

    pl.semaphore_signal(barrier, inc=1, device_id={"inner": mate}, device_id_type=MESH)

    loads = [
        pltpu.make_async_copy(src, dst, in_sem.at[i])
        for i, (src, dst) in enumerate(
            (
                (idx_hbm, slots.at[0]), (val_hbm, slots.at[1]),
                (k_ref, kv.at[0]), (v_ref, kv.at[1]), (q_ref, qd.at[0]), (do_ref, qd.at[1]),
            )
        )
    ]
    for load in loads:
        load.start()

    waits = me == middle - 1

    def answer(j, _):
        pl.semaphore_signal(ready.at[me], inc=1, device_id={"seq": j}, device_id_type=MESH)
        return 0

    @pl.when(jnp.logical_not(waits))
    def _():
        pl.semaphore_wait(barrier, me + 1)
        lax.fori_loop(0, jnp.where(me == middle, me - 1, me), answer, 0)

    loads[0].wait()
    loads[1].wait()
    picked = jnp.where(slots[1] > 0, slots[0], -1)
    block = iota((lanes, total), 0)
    hit = jnp.zeros((lanes, total), F32)
    for t in range(topk):
        hit = jnp.where(picked[t : t + 1, :] == block, 1.0, hit)
    eye = jnp.where(iota((total, total), 0) == iota((total, total), 1), 1.0, 0.0).astype(BF)
    sel[...] = dot_nt(eye, hit.astype(BF))
    nb_shift = log2(nb)
    tri_r = iota((lanes, lanes), 0)
    tri_c = iota((lanes, lanes), 1)
    tri = jnp.where(
        (tri_r < tri_c)
        & (lax.shift_right_logical(tri_r, nb_shift) == lax.shift_right_logical(tri_c, nb_shift)),
        1.0,
        0.0,
    ).astype(BF)

    def ranks(run):
        rows = sel[pl.ds(pl.multiple_of(run * nb, nb), nb), :]
        present = jnp.max(rows, axis=0, keepdims=True)
        rank = dot(jnp.broadcast_to(present, (8, lanes)).astype(BF), tri)[0:1, :]
        return rows, present, rank

    def expand(axis):
        shape = (lanes, own_rows) if axis else (own_rows, lanes)
        block = lax.shift_right_logical(iota(shape, axis), log2(BLK)) + me * nb
        return jnp.where(block == iota(shape, 1 - axis), 1.0, 0.0).astype(BF)

    spread = expand(1)
    spread_t = expand(0)

    def send_a(r):
        return pltpu.make_async_remote_copy(
            src_ref=stage.at[r],
            dst_ref=pool.at[mate, pl.ds(pl.multiple_of(me * chunk, chunk), chunk)],
            send_sem=a_send.at[r],
            recv_sem=a_recv.at[me],
            device_id={"seq": r},
            device_id_type=MESH,
        )

    def code_of(r):
        _, present, rank = ranks(r)
        return jnp.broadcast_to(jnp.where(present > 0.5, rank, -8.0), (8, lanes)).astype(BF)

    def scatter_of(code):
        down = dot_nt(spread_t, jnp.broadcast_to(code[0:1, :], (chunk, lanes)))
        down = down.astype(jnp.int32) * BLK + (iota((own_rows, chunk), 0) & (BLK - 1))
        return jnp.where(down == iota((own_rows, chunk), 1), 1.0, 0.0).astype(BF)

    loads[2].wait()
    loads[3].wait()

    def choose(j, _):
        r = me + 1 + j

        @pl.when(waits & (j == 1))
        def _():
            pl.semaphore_wait(barrier, me + 2)
            lax.fori_loop(0, me, answer, 0)
            send_a(r - 1).start()

        code = code_of(r)
        across = dot(code, spread)[0:1, :].astype(jnp.int32) * BLK
        across = across + (iota((1, own_rows), 1) & (BLK - 1))
        pick = jnp.where(across == iota((chunk, own_rows), 0), 1.0, 0.0).astype(BF)
        stage[r] = dot(pick, kv[mate]).astype(BF)
        return 0

    lax.fori_loop(0, S - 1 - me, choose, 0)

    def give(j, _):
        r = me + 1 + j
        pl.semaphore_wait(ready.at[r], 1)
        send_a(r).start()
        return 0

    lax.fori_loop(jnp.where(waits, 1, 0), S - 1 - me, give, 0)

    mine, present, rank = ranks(me)
    block_row = iota((1, lanes), 1)
    run_row = lax.shift_right_logical(block_row, nb_shift)
    place = jnp.where(
        run_row < me,
        run_row * CAP + rank.astype(jnp.int32),
        (S - 1) * CAP + (block_row & (nb - 1)),
    )
    place = jnp.where((present > 0.5) & (run_row <= me), place, -1)
    table = jnp.where(place == iota((slot_lanes, lanes), 0), 1.0, 0.0).astype(BF)
    bias = jnp.where(dot_nt(mine.astype(BF), table) > 0.5, 0.0, NEG)
    loads[4].wait()
    loads[5].wait()
    for b in range(nb):
        rows = pl.ds(b * rows_b, rows_b)
        qaug[rows, 0:width] = qd[0, rows, :]
        qaug[rows, width:] = jnp.broadcast_to(bias[b : b + 1, :], (rows_b, slot_lanes)).astype(BF)
    nkeys = oh.shape[0]
    oh[...] = jnp.where(
        lax.shift_right_logical(iota((nkeys, slot_lanes), 0), log2(BLK))
        == iota((nkeys, slot_lanes), 1),
        1.0,
        0.0,
    ).astype(BF)
    kt[:, nrem:] = kv[0].astype(F32).T.astype(BF)

    pair = 2 if nb % 2 == 0 else 1

    def own_count(b):
        return (b // pair + 1) * pair * BLK

    def fold(x, how):
        return how(how(x.reshape(-1, 8, rows_b), axis=0), axis=0, keepdims=True)

    def block_rows(b):
        return pl.ds(b * rows_b, rows_b)

    def soft(b, n, slot, keys_at):
        e = jnp.exp2((s_buf[b, 0:n, :] - st_m[slot, b : b + 1, :]) * c2)
        st_l[slot, b : b + 1, :] = fold(e, jnp.sum)
        pd[1, keys_at, block_rows(b)] = e.astype(BF)

    def lean(b, slot, turned_v, keys_at):
        out = dot(turned_v, pd[1, keys_at, block_rows(b)])
        st_d[slot, b : b + 1, :] = fold(out * dot_t[:, block_rows(b)], jnp.sum)

    def probs(b, slot, keys_at):
        return pd[1, keys_at, block_rows(b)].astype(F32) * st_l[slot, b : b + 1, :]

    def grads(b, p, vals, keys_at, delta):
        rows = block_rows(b)
        dp = dot_nt(vals, qd[1, rows, :])
        pd[0, keys_at, rows] = (p * (dp - delta[b : b + 1, :])).astype(BF)

    own_slot = S - 1
    st_m[...] = jnp.full((S, nb, rows_b), NEG, F32)
    st_l[...] = jnp.zeros((S, nb, rows_b), F32)
    st_d[...] = jnp.zeros((S, nb, rows_b), F32)
    vt_own[...] = kv[1].astype(F32).T.astype(BF)

    def own_scores(b):
        n = own_count(b)
        ka = jnp.concatenate([kv[0, 0:n, :], oh[nrem : nrem + n, :]], axis=1)
        s = dot_nt(ka, qaug[block_rows(b), :])
        lo, hi = b * BLK, (b + 1) * BLK
        key = iota((BLK, rows_b), 0)
        query = lax.shift_right_logical(iota((BLK, rows_b), 1), log2(heads))
        parts = [jnp.where(key > query, NEG, s[lo:hi])]
        if lo:
            parts.insert(0, s[0:lo])
        if hi < n:
            parts.append(s[hi:n])
        s = jnp.concatenate(parts, axis=0)
        s_buf[b, 0:n, :] = s
        st_m[own_slot, b : b + 1, :] = fold(s, jnp.max)

    def ahead(first, then):
        first(0)
        for b in range(nb):
            if b + 1 < nb:
                first(b + 1)
            then(b)

    ahead(own_scores, lambda b: soft(b, own_count(b), own_slot, pl.ds(nrem, own_count(b))))
    for b in range(nb):
        rows = block_rows(b)
        dot_t[:, rows] = qd[1, rows, :].astype(F32).T
        n = own_count(b)
        lean(b, own_slot, vt_own[:, 0:n], pl.ds(nrem, n))

    if pre:

        def scatters(j, _):
            r = me + 1 + j
            wt[r] = scatter_of(code_of(r))
            return 0

        lax.fori_loop(0, S - 1 - me, scatters, 0)

    def blank(s, _):
        at = pl.ds(pl.multiple_of(s * chunk, chunk), chunk)
        pool[0, at, :] = jnp.zeros((chunk, width), BF)
        pool[1, at, :] = jnp.zeros((chunk, width), BF)
        for b in range(nb):
            pd[0, at, block_rows(b)] = jnp.zeros((chunk, rows_b), BF)
        return 0

    lax.fori_loop(me, S - 1, blank, 0)

    def pool_at(kind, s):
        return pool.at[kind, pl.ds(pl.multiple_of(s * chunk, chunk), chunk)]

    def recv_a(s):
        return pltpu.make_async_remote_copy(
            src_ref=stage.at[s],
            dst_ref=pool_at(mate, s),
            send_sem=a_send.at[s],
            recv_sem=a_recv.at[s],
            device_id={"seq": s},
            device_id_type=MESH,
        )

    def forward(kind, s):
        return pltpu.make_async_remote_copy(
            src_ref=pool_at(kind, s),
            dst_ref=pool_at(kind, s),
            send_sem=f_send.at[s],
            recv_sem=f_recv.at[s],
            device_id={"inner": mate},
            device_id_type=MESH,
        )

    def keys_of(s):
        return pl.ds(pl.multiple_of(s * chunk, chunk), chunk)

    def weigh(s):
        at = keys_of(s)

        def scores(b):
            ka = jnp.concatenate([pool[0, at, :], oh[at, :]], axis=1)
            part = dot_nt(ka, qaug[block_rows(b), :])
            s_buf[b, 0:chunk, :] = part
            st_m[s, b : b + 1, :] = fold(part, jnp.max)

        ahead(scores, lambda b: soft(b, chunk, s, at))

    def average(s):
        at = keys_of(s)
        turned_v = pool[1, at, :].astype(F32).T.astype(BF)
        for b in range(nb):
            lean(b, s, turned_v, at)

    def land(s):
        recv_a(s).wait_recv()
        forward(mate, s).start()

    def keys_in(s):
        @pl.when(core == 1)
        def _():
            land(s)

        @pl.when(core == 0)
        def _():
            forward(core, s).wait_recv()

        weigh(s)

    def values_in(s):
        @pl.when(core == 1)
        def _():
            forward(core, s).wait_recv()

        average(s)

    def down(first, body):
        def at(j, _):
            body(me - 1 - j)
            return 0

        lax.fori_loop(first, me, at, 0)

    @pl.when(me > 0)
    def _():
        keys_in(me - 1)

    early = jnp.where(me == S - 1, 1, 0)

    @pl.when(early == 1)
    def _():
        @pl.when(core == 0)
        def _():
            land(me - 1)

        values_in(me - 1)

    @pl.when(core == 0)
    def _():
        down(early, land)

    down(1, keys_in)
    down(early, values_in)

    top = st_m[0]
    for s in range(1, S):
        top = jnp.maximum(top, st_m[s])
    mass = jnp.zeros((nb, rows_b), F32)
    delta = jnp.zeros((nb, rows_b), F32)
    for s in range(S):
        w = jnp.exp2((st_m[s] - top) * c2)
        st_m[s] = w
        mass += w * st_l[s]
        delta += w * st_d[s]
    inv = 1.0 / mass
    st_d[0] = delta * inv
    for s in range(S):
        st_l[s] = st_m[s] * inv

    def scale_of(kind):
        return jnp.where(kind == 0, scaling, 1.0).astype(F32)

    def swap(s):
        return pltpu.make_async_remote_copy(
            src_ref=terms.at[s, mate],
            dst_ref=xrecv.at[s],
            send_sem=x_send.at[s],
            recv_sem=x_recv.at[s],
            device_id={"inner": mate},
            device_id_type=MESH,
        )

    def give_back(s):
        return pltpu.make_async_remote_copy(
            src_ref=tsend.at[s],
            dst_ref=trecv.at[me],
            send_sem=t_send.at[s],
            recv_sem=t_recv.at[me],
            device_id={"seq": s},
            device_id_type=MESH,
        )

    def finish(s):
        swap(s).wait_recv()
        tsend[s] = (terms[s, core] + xrecv[s]).astype(BF)
        give_back(s).start()

    def remote(s, _):
        at = keys_of(s)
        delta = st_d[0]
        for b in range(nb):
            p_run[:, block_rows(b)] = probs(b, s, at).astype(BF)
        terms[s, 1] = dot(p_run[...], qd[1])

        @pl.when(core == 0)
        def _():
            swap(s).start()

        @pl.when(s > 0)
        def _():
            finish(s - 1)

        for b in range(nb):
            grads(b, probs(b, s, at), pool[1, at, :], at, delta)
        terms[s, 0] = dot(pd[0, at, :], qd[0]) * scaling

        @pl.when(core == 1)
        def _():
            swap(s).start()

        return 0

    lax.fori_loop(0, me, remote, 0)

    @pl.when(me > 0)
    def _():
        finish(me - 1)

    own_swap = pltpu.make_async_remote_copy(
        src_ref=ox_send,
        dst_ref=ox_recv,
        send_sem=o_sem.at[0],
        recv_sem=o_sem.at[1],
        device_id={"inner": mate},
        device_id_type=MESH,
    )

    def own_terms(kind, target):
        for c in range(0, nb, pair):
            n = pair * BLK
            lo = c * rows_b
            target[c * BLK : c * BLK + n, :] = (
                dot(pd[kind, nrem + c * BLK : nrem + c * BLK + n, lo:], qd[kind, lo:, :])
                * scale_of(kind)
            )

    delta = st_d[0]
    for b in range(nb):
        n = own_count(b)
        p = probs(b, own_slot, pl.ds(nrem, n))
        pd[1, pl.ds(nrem, n), block_rows(b)] = p.astype(BF)
        grads(b, p, kv[1, 0:n, :], pl.ds(nrem, n), delta)
    own_terms(mate, ox_send)
    own_swap.start()
    own_terms(core, acc)

    for s in range(S - 1):
        kt[:, s * chunk : (s + 1) * chunk] = (
            pool[0, s * chunk : (s + 1) * chunk, :].astype(F32).T.astype(BF)
        )
    for b in range(nb):
        rows = pl.ds(b * rows_b, rows_b)
        n = nrem + own_count(b)
        turned = dot(kt[:, 0:n], pd[0, 0:n, rows]) * scaling
        dq_ref[rows, :] = turned.T.astype(BF)

    own_swap.wait_recv()
    acc[...] += ox_recv[...]

    def gather(j, _):
        r = me + 1 + j
        pltpu.make_async_remote_copy(
            src_ref=tsend.at[r],
            dst_ref=trecv.at[r],
            send_sem=t_send.at[r],
            recv_sem=t_recv.at[r],
            device_id={"seq": r},
            device_id_type=MESH,
        ).wait_recv()
        acc[...] += dot(wt[r] if pre else scatter_of(code_of(r)), trecv[r])
        return 0

    lax.fori_loop(0, S - 1 - me, gather, 0)

    def last(ref):
        return pltpu.make_async_remote_copy(
            src_ref=ref,
            dst_ref=ref,
            send_sem=r_sem.at[0],
            recv_sem=r_sem.at[1],
            device_id={"inner": mate},
            device_id_type=MESH,
        )

    @pl.when(core == 0)
    def _():
        dk_ref[...] = acc[...].astype(BF)
        last(dk_ref).start()

    @pl.when(core == 1)
    def _():
        dv_ref[...] = acc[...].astype(BF)
        last(dv_ref).start()

    def close_up(j, _):
        send_a(me + 1 + j).wait_send()
        return 0

    lax.fori_loop(0, S - 1 - me, close_up, 0)

    def close_down(s, _):
        forward(mate, s).wait_send()
        swap(s).wait_send()
        give_back(s).wait_send()
        return 0

    lax.fori_loop(0, me, close_down, 0)
    own_swap.wait_send()

    @pl.when(core == 0)
    def _():
        last(dk_ref).wait_send()
        last(dv_ref).wait_recv()

    @pl.when(core == 1)
    def _():
        last(dv_ref).wait_send()
        last(dk_ref).wait_recv()


def place_kernel(*refs):
    n = len(refs) // 2
    moves = [pltpu.make_async_copy(refs[i], refs[n + i], refs[-1].at[i]) for i in range(n)]
    for move in moves:
        move.start()
    for move in moves:
        move.wait()


def place(*arrays):
    return pl.pallas_call(
        place_kernel,
        out_shape=tuple(jax.ShapeDtypeStruct(a.shape, a.dtype) for a in arrays),
        in_specs=[pl.BlockSpec(memory_space=pltpu.VMEM)] * len(arrays),
        out_specs=(pl.BlockSpec(memory_space=pl.ANY),) * len(arrays),
        scratch_shapes=[pltpu.SemaphoreType.DMA((len(arrays),))],
        compiler_params=pltpu.CompilerParams(vmem_limit_bytes=65536),
    )(*(pltpu.with_memory_space_constraint(a, pltpu.VMEM) for a in arrays))


def per_device(queries, grad_out, keys, values, indices, valid):
    tokens, _, heads, width = queries.shape
    S = lax.axis_size("seq")
    total, topk = indices.shape[1:]
    nb = tokens // BLK
    chunk = CAP * BLK
    nrem = (S - 1) * chunk
    own_rows = tokens
    nkeys = nrem + own_rows
    rows = tokens * heads
    rows_b = BLK * heads
    lanes = -(-total // 128) * 128
    slot_lanes = -(-(nkeys // BLK) // 128) * 128
    pre = S <= 4
    cfg = (S, heads, nb, total, topk, width, pre)
    vmem = pl.BlockSpec(memory_space=pltpu.VMEM)
    hbm = pl.BlockSpec(memory_space=pl.ANY)
    dma = pltpu.SemaphoreType.DMA
    dq, dk, dv = pl.pallas_call(
        functools.partial(kernel, cfg),
        out_shape=(
            pltpu.VMEM((rows, width), BF),
            pltpu.VMEM((own_rows, width), BF),
            pltpu.VMEM((own_rows, width), BF),
        ),
        in_specs=[hbm] * 6,
        out_specs=(vmem, vmem, vmem),
        scratch_shapes=[
            pltpu.VMEM((total, lanes), F32),
            pltpu.VMEM((rows, width + slot_lanes), BF),
            pltpu.VMEM((2, rows, width), BF),
            pltpu.VMEM((2, own_rows, width), BF),
            pltpu.VMEM((nkeys, slot_lanes), BF),
            pltpu.VMEM((width, nkeys), BF),
            pltpu.VMEM((width, own_rows), BF),
            pltpu.VMEM((width, rows), F32),
            pltpu.VMEM((S, chunk, width), BF),
            pltpu.VMEM((2, nrem, width), BF),
            pltpu.VMEM((S if pre else 1, own_rows, chunk), BF),
            pltpu.VMEM((nb, max(own_rows, chunk), rows_b), F32),
            pltpu.VMEM((2, nkeys, rows), BF),
            pltpu.VMEM((chunk, rows), BF),
            pltpu.VMEM((S, 2, chunk, width), F32),
            pltpu.VMEM((S, chunk, width), F32),
            pltpu.VMEM((S, chunk, width), BF),
            pltpu.VMEM((S, chunk, width), BF),
            pltpu.VMEM((own_rows, width), F32),
            pltpu.VMEM((own_rows, width), F32),
            pltpu.VMEM((own_rows, width), F32),
            dma((S,)), dma((S,)), dma((S,)), dma((S,)), dma((S,)), dma((S,)),
            dma((S,)), dma((S,)), dma((2,)), dma((2,)),
            dma((6,)),
            pltpu.SemaphoreType.REGULAR((S,)),
            pltpu.VMEM((2, topk, total), jnp.int32),
            pltpu.VMEM((S, nb, rows_b), F32),
            pltpu.VMEM((S, nb, rows_b), F32),
            pltpu.VMEM((S, nb, rows_b), F32),
        ],
        compiler_params=pltpu.CompilerParams(
            collective_id=0, has_side_effects=True, vmem_limit_bytes=67043328 - 6 * own_rows * width * 2 - 4096
        ),
    )(
        queries.reshape(rows, width),
        grad_out.reshape(rows, width),
        keys.reshape(own_rows, width),
        values.reshape(own_rows, width),
        indices[0].T,
        valid[0].T,
    )
    dq, dk, dv = place(dq, dk, dv)
    return (
        dq.reshape(tokens, 1, heads, width),
        dk.reshape(tokens, 1, width),
        dv.reshape(tokens, 1, width),
    )


def solution(mesh):
    return jax.shard_map(
        per_device,
        mesh=mesh,
        in_specs=(
            P(("groups", "seq"), "head", "inner", None),
            P(("groups", "seq"), "head", "inner", None),
            P(("groups", "seq"), "head", None),
            P(("groups", "seq"), "head", None),
            P("head", "groups", None),
            P("head", "groups", None),
        ),
        out_specs=(
            P(("groups", "seq"), "head", "inner", None),
            P(("groups", "seq"), "head", None),
            P(("groups", "seq"), "head", None),
        ),
        check_vma=False,
    )
```

```python
import functools
import math

import jax
import jax.numpy as jnp
from jax import lax
from jax.experimental import pallas as pl
from jax.experimental.pallas import tpu as pltpu
from jax.sharding import PartitionSpec as P

BLK = 64
CAP = 4
MESH = pl.DeviceIdType.MESH
NEG = -1e30
NT = (((1,), (1,)), ((), ()))
F32 = jnp.float32
BF = jnp.bfloat16


def dot(a, b):
    return jnp.dot(a, b, preferred_element_type=F32)


def dot_nt(a, b):
    return lax.dot_general(a, b, NT, preferred_element_type=F32)


def log2(n):
    shift = n.bit_length() - 1
    assert 1 << shift == n
    return shift


def iota(shape, axis):
    return lax.broadcasted_iota(jnp.int32, shape, axis)


def kernel(
    cfg,
    q_ref, do_ref, k_ref, v_ref, idx_hbm, val_hbm,
    dq_ref, dk_ref, dv_ref,
    sel, qaug, qd, kv, oh, kt, vt, vt_own, dot_t, do_t, stage, pool, wt,
    s_buf, pd, p_run, terms, xrecv, tsend, trecv, ox_send, ox_recv, acc,
    a_send, a_recv, f_send, f_recv, x_send, x_recv, t_send, t_recv, o_sem, r_sem, in_sem,
    ready, slots, st_m, st_l, st_d,
):
    S, heads, nb, total, topk, width, pre = cfg
    me = lax.axis_index("seq")
    core = lax.axis_index("inner")
    mate = 1 - core
    chunk = CAP * BLK
    nrem = (S - 1) * chunk
    rows_b = BLK * heads
    own_rows = nb * BLK
    lanes = sel.shape[1]
    slot_lanes = oh.shape[1]
    scaling = 1.0 / math.sqrt(width)
    c2 = scaling * math.log2(math.e)

    barrier = pltpu.get_barrier_semaphore()

    def hello(j, _):
        pl.semaphore_signal(barrier, inc=1, device_id={"seq": S - 1 - j}, device_id_type=MESH)
        return 0

    lax.fori_loop(0, S - 1 - me, hello, 0)
    middle = S // 2

    @pl.when(me == middle)
    def _():
        pl.semaphore_signal(barrier, inc=1, device_id={"seq": middle - 1}, device_id_type=MESH)

    pl.semaphore_signal(barrier, inc=1, device_id={"inner": mate}, device_id_type=MESH)

    loads = [
        pltpu.make_async_copy(src, dst, in_sem.at[i])
        for i, (src, dst) in enumerate(
            (
                (idx_hbm, slots.at[0]), (val_hbm, slots.at[1]),
                (k_ref, kv.at[0]), (v_ref, kv.at[1]), (q_ref, qd.at[0]), (do_ref, qd.at[1]),
            )
        )
    ]
    for load in loads:
        load.start()

    waits = me == middle - 1

    def answer(j, _):
        pl.semaphore_signal(ready.at[me], inc=1, device_id={"seq": j}, device_id_type=MESH)
        return 0

    @pl.when(jnp.logical_not(waits))
    def _():
        pl.semaphore_wait(barrier, me + 1)
        lax.fori_loop(0, jnp.where(me == middle, me - 1, me), answer, 0)

    loads[0].wait()
    loads[1].wait()
    picked = jnp.where(slots[1] > 0, slots[0], -1)
    block = iota((lanes, total), 0)
    hit = jnp.zeros((lanes, total), F32)
    for t in range(topk):
        hit = jnp.where(picked[t : t + 1, :] == block, 1.0, hit)
    eye = jnp.where(iota((total, total), 0) == iota((total, total), 1), 1.0, 0.0).astype(BF)
    sel[...] = dot_nt(eye, hit.astype(BF))
    nb_shift = log2(nb)
    tri_r = iota((lanes, lanes), 0)
    tri_c = iota((lanes, lanes), 1)
    tri = jnp.where(
        (tri_r < tri_c)
        & (lax.shift_right_logical(tri_r, nb_shift) == lax.shift_right_logical(tri_c, nb_shift)),
        1.0,
        0.0,
    ).astype(BF)

    def ranks(run):
        rows = sel[pl.ds(pl.multiple_of(run * nb, nb), nb), :]
        present = jnp.max(rows, axis=0, keepdims=True)
        rank = dot(jnp.broadcast_to(present, (8, lanes)).astype(BF), tri)[0:1, :]
        return rows, present, rank

    def expand(axis):
        shape = (lanes, own_rows) if axis else (own_rows, lanes)
        block = lax.shift_right_logical(iota(shape, axis), log2(BLK)) + me * nb
        return jnp.where(block == iota(shape, 1 - axis), 1.0, 0.0).astype(BF)

    spread = expand(1)
    spread_t = expand(0)

    def send_a(r):
        return pltpu.make_async_remote_copy(
            src_ref=stage.at[r],
            dst_ref=pool.at[mate, pl.ds(pl.multiple_of(me * chunk, chunk), chunk)],
            send_sem=a_send.at[r],
            recv_sem=a_recv.at[me],
            device_id={"seq": r},
            device_id_type=MESH,
        )

    def code_of(r):
        _, present, rank = ranks(r)
        return jnp.broadcast_to(jnp.where(present > 0.5, rank, -8.0), (8, lanes)).astype(BF)

    def scatter_of(code):
        down = dot_nt(spread_t, jnp.broadcast_to(code[0:1, :], (chunk, lanes)))
        down = down.astype(jnp.int32) * BLK + (iota((own_rows, chunk), 0) & (BLK - 1))
        return jnp.where(down == iota((own_rows, chunk), 1), 1.0, 0.0).astype(BF)

    loads[2].wait()
    loads[3].wait()

    def choose(j, _):
        r = me + 1 + j

        @pl.when(waits & (j == 1))
        def _():
            pl.semaphore_wait(barrier, me + 2)
            lax.fori_loop(0, me, answer, 0)
            send_a(r - 1).start()

        code = code_of(r)
        across = dot(code, spread)[0:1, :].astype(jnp.int32) * BLK
        across = across + (iota((1, own_rows), 1) & (BLK - 1))
        pick = jnp.where(across == iota((chunk, own_rows), 0), 1.0, 0.0).astype(BF)
        stage[r] = dot(pick, kv[mate]).astype(BF)
        return 0

    lax.fori_loop(0, S - 1 - me, choose, 0)

    def give(j, _):
        r = me + 1 + j
        pl.semaphore_wait(ready.at[r], 1)
        send_a(r).start()
        return 0

    lax.fori_loop(jnp.where(waits, 1, 0), S - 1 - me, give, 0)

    mine, present, rank = ranks(me)
    block_row = iota((1, lanes), 1)
    run_row = lax.shift_right_logical(block_row, nb_shift)
    place = jnp.where(
        run_row < me,
        run_row * CAP + rank.astype(jnp.int32),
        (S - 1) * CAP + (block_row & (nb - 1)),
    )
    place = jnp.where((present > 0.5) & (run_row <= me), place, -1)
    table = jnp.where(place == iota((slot_lanes, lanes), 0), 1.0, 0.0).astype(BF)
    bias = jnp.where(dot_nt(table, mine.astype(BF)) > 0.5, 0.0, NEG)
    loads[4].wait()
    loads[5].wait()
    for b in range(nb):
        rows = pl.ds(b * rows_b, rows_b)
        qaug[0:width, rows] = qd[0, rows, :].astype(F32).T.astype(BF)
        qaug[width:, rows] = jnp.broadcast_to(bias[:, b : b + 1], (slot_lanes, rows_b)).astype(BF)
    nkeys = oh.shape[0]
    oh[...] = jnp.where(
        lax.shift_right_logical(iota((nkeys, slot_lanes), 0), log2(BLK))
        == iota((nkeys, slot_lanes), 1),
        1.0,
        0.0,
    ).astype(BF)
    kt[:, nrem:] = kv[0].astype(F32).T.astype(BF)

    pair = 2 if nb % 2 == 0 else 1

    def own_count(b):
        return (b // pair + 1) * pair * BLK

    def fold(x, how):
        return how(how(x.reshape(-1, 8, rows_b), axis=0), axis=0, keepdims=True)

    def block_rows(b):
        return pl.ds(b * rows_b, rows_b)

    def soft(b, n, slot, keys_at):
        e = jnp.exp2((s_buf[b, 0:n, :] - st_m[slot, b : b + 1, :]) * c2)
        pd[1, keys_at, block_rows(b)] = e.astype(BF)

    def lean(b, slot, turned_v, keys_at):
        ones = jnp.ones((16, turned_v.shape[1]), BF)
        out = dot(jnp.concatenate([turned_v, ones], axis=0), pd[1, keys_at, block_rows(b)])
        st_l[slot, b : b + 1, :] = out[width : width + 1]
        st_d[slot, b : b + 1, :] = fold(out[0:width] * dot_t[:, block_rows(b)], jnp.sum)

    def probs(b, slot, keys_at):
        return pd[1, keys_at, block_rows(b)].astype(F32) * st_l[slot, b : b + 1, :]

    def grads(b, p, vals, keys_at, delta):
        rows = block_rows(b)
        dp = dot(vals, do_t[:, rows])
        pd[0, keys_at, rows] = (p * (dp - delta[b : b + 1, :])).astype(BF)

    own_slot = S - 1
    st_m[...] = jnp.full((S, nb, rows_b), NEG, F32)
    st_l[...] = jnp.zeros((S, nb, rows_b), F32)
    st_d[...] = jnp.zeros((S, nb, rows_b), F32)
    vt_own[...] = kv[1].astype(F32).T.astype(BF)

    def own_scores(b):
        n = own_count(b)
        ka = jnp.concatenate([kv[0, 0:n, :], oh[nrem : nrem + n, :]], axis=1)
        s = dot(ka, qaug[:, block_rows(b)])
        lo, hi = b * BLK, (b + 1) * BLK
        key = iota((BLK, rows_b), 0)
        query = lax.shift_right_logical(iota((BLK, rows_b), 1), log2(heads))
        parts = [jnp.where(key > query, NEG, s[lo:hi])]
        if lo:
            parts.insert(0, s[0:lo])
        if hi < n:
            parts.append(s[hi:n])
        s = jnp.concatenate(parts, axis=0)
        s_buf[b, 0:n, :] = s
        st_m[own_slot, b : b + 1, :] = fold(s, jnp.max)

    def ahead(first, then):
        first(0)
        for b in range(nb):
            if b + 1 < nb:
                first(b + 1)
            then(b)

    ahead(own_scores, lambda b: soft(b, own_count(b), own_slot, pl.ds(nrem, own_count(b))))
    for b in range(nb):
        rows = block_rows(b)
        turned_do = qd[1, rows, :].astype(F32).T
        dot_t[:, rows] = turned_do
        do_t[:, rows] = turned_do.astype(BF)
        n = own_count(b)
        lean(b, own_slot, vt_own[:, 0:n], pl.ds(nrem, n))

    if pre:

        def scatters(j, _):
            r = me + 1 + j
            wt[r] = scatter_of(code_of(r))
            return 0

        lax.fori_loop(0, S - 1 - me, scatters, 0)

    def blank(s, _):
        at = pl.ds(pl.multiple_of(s * chunk, chunk), chunk)
        pool[0, at, :] = jnp.zeros((chunk, width), BF)
        pool[1, at, :] = jnp.zeros((chunk, width), BF)
        for b in range(nb):
            pd[0, at, block_rows(b)] = jnp.zeros((chunk, rows_b), BF)
        return 0

    lax.fori_loop(me, S - 1, blank, 0)

    def pool_at(kind, s):
        return pool.at[kind, pl.ds(pl.multiple_of(s * chunk, chunk), chunk)]

    def recv_a(s):
        return pltpu.make_async_remote_copy(
            src_ref=stage.at[s],
            dst_ref=pool_at(mate, s),
            send_sem=a_send.at[s],
            recv_sem=a_recv.at[s],
            device_id={"seq": s},
            device_id_type=MESH,
        )

    def forward(kind, s):
        return pltpu.make_async_remote_copy(
            src_ref=pool_at(kind, s),
            dst_ref=pool_at(kind, s),
            send_sem=f_send.at[s],
            recv_sem=f_recv.at[s],
            device_id={"inner": mate},
            device_id_type=MESH,
        )

    def keys_of(s):
        return pl.ds(pl.multiple_of(s * chunk, chunk), chunk)

    def weigh(s):
        at = keys_of(s)

        def scores(b):
            ka = jnp.concatenate([pool[0, at, :], oh[at, :]], axis=1)
            part = dot(ka, qaug[:, block_rows(b)])
            s_buf[b, 0:chunk, :] = part
            st_m[s, b : b + 1, :] = fold(part, jnp.max)

        ahead(scores, lambda b: soft(b, chunk, s, at))

    def average(s):
        at = keys_of(s)
        for b in range(nb):
            lean(b, s, vt[s], at)

    def turn(s):
        vt[s] = pool[1, keys_of(s), :].astype(F32).T.astype(BF)

    def land(s):
        recv_a(s).wait_recv()
        forward(mate, s).start()

    def land_values(s):
        land(s)
        turn(s)

    def keys_in(s):
        @pl.when(core == 1)
        def _():
            land(s)

        @pl.when(core == 0)
        def _():
            forward(core, s).wait_recv()

        weigh(s)

    def values_in(s):
        @pl.when(core == 1)
        def _():
            forward(core, s).wait_recv()
            turn(s)

        average(s)

    def down(first, body):
        def at(j, _):
            body(me - 1 - j)
            return 0

        lax.fori_loop(first, me, at, 0)

    @pl.when(me > 0)
    def _():
        keys_in(me - 1)

    early = jnp.where(me == S - 1, 1, 0)

    @pl.when(early == 1)
    def _():
        @pl.when(core == 0)
        def _():
            land_values(me - 1)

        values_in(me - 1)

    @pl.when(core == 0)
    def _():
        down(early, land_values)

    down(1, keys_in)
    down(early, values_in)

    top = st_m[0]
    for s in range(1, S):
        top = jnp.maximum(top, st_m[s])
    mass = jnp.zeros((nb, rows_b), F32)
    delta = jnp.zeros((nb, rows_b), F32)
    for s in range(S):
        w = jnp.exp2((st_m[s] - top) * c2)
        st_m[s] = w
        mass += w * st_l[s]
        delta += w * st_d[s]
    inv = 1.0 / mass
    st_d[0] = delta * inv
    for s in range(S):
        st_l[s] = st_m[s] * inv

    def scale_of(kind):
        return jnp.where(kind == 0, scaling, 1.0).astype(F32)

    def swap(s):
        return pltpu.make_async_remote_copy(
            src_ref=terms.at[s, mate],
            dst_ref=xrecv.at[s],
            send_sem=x_send.at[s],
            recv_sem=x_recv.at[s],
            device_id={"inner": mate},
            device_id_type=MESH,
        )

    def give_back(s):
        return pltpu.make_async_remote_copy(
            src_ref=tsend.at[s],
            dst_ref=trecv.at[me],
            send_sem=t_send.at[s],
            recv_sem=t_recv.at[me],
            device_id={"seq": s},
            device_id_type=MESH,
        )

    def finish(s):
        swap(s).wait_recv()
        tsend[s] = (terms[s, core] + xrecv[s]).astype(BF)
        give_back(s).start()

    def remote(s, _):
        at = keys_of(s)
        delta = st_d[0]
        for b in range(nb):
            p_run[:, block_rows(b)] = probs(b, s, at).astype(BF)
        terms[s, 1] = dot(p_run[...], qd[1])

        @pl.when(core == 0)
        def _():
            swap(s).start()

        @pl.when(s > 0)
        def _():
            finish(s - 1)

        for b in range(nb):
            grads(b, probs(b, s, at), pool[1, at, :], at, delta)
        terms[s, 0] = dot(pd[0, at, :], qd[0]) * scaling

        @pl.when(core == 1)
        def _():
            swap(s).start()

        return 0

    lax.fori_loop(0, me, remote, 0)

    @pl.when(me > 0)
    def _():
        finish(me - 1)

    own_swap = pltpu.make_async_remote_copy(
        src_ref=ox_send,
        dst_ref=ox_recv,
        send_sem=o_sem.at[0],
        recv_sem=o_sem.at[1],
        device_id={"inner": mate},
        device_id_type=MESH,
    )

    def own_terms(kind, target):
        for c in range(0, nb, pair):
            n = pair * BLK
            lo = c * rows_b
            target[c * BLK : c * BLK + n, :] = (
                dot(pd[kind, nrem + c * BLK : nrem + c * BLK + n, lo:], qd[kind, lo:, :])
                * scale_of(kind)
            )

    delta = st_d[0]
    for b in range(nb):
        n = own_count(b)
        p = probs(b, own_slot, pl.ds(nrem, n))
        pd[1, pl.ds(nrem, n), block_rows(b)] = p.astype(BF)
        grads(b, p, kv[1, 0:n, :], pl.ds(nrem, n), delta)
    own_terms(mate, ox_send)
    own_swap.start()
    own_terms(core, acc)

    for s in range(S - 1):
        kt[:, s * chunk : (s + 1) * chunk] = (
            pool[0, s * chunk : (s + 1) * chunk, :].astype(F32).T.astype(BF)
        )
    for b in range(nb):
        rows = pl.ds(b * rows_b, rows_b)
        n = nrem + own_count(b)
        turned = dot(kt[:, 0:n], pd[0, 0:n, rows]) * scaling
        dq_ref[rows, :] = turned.T.astype(BF)

    own_swap.wait_recv()
    acc[...] += ox_recv[...]

    def gather(j, _):
        r = me + 1 + j
        pltpu.make_async_remote_copy(
            src_ref=tsend.at[r],
            dst_ref=trecv.at[r],
            send_sem=t_send.at[r],
            recv_sem=t_recv.at[r],
            device_id={"seq": r},
            device_id_type=MESH,
        ).wait_recv()
        acc[...] += dot(wt[r] if pre else scatter_of(code_of(r)), trecv[r])
        return 0

    lax.fori_loop(0, S - 1 - me, gather, 0)

    def last(ref):
        return pltpu.make_async_remote_copy(
            src_ref=ref,
            dst_ref=ref,
            send_sem=r_sem.at[0],
            recv_sem=r_sem.at[1],
            device_id={"inner": mate},
            device_id_type=MESH,
        )

    @pl.when(core == 0)
    def _():
        dk_ref[...] = acc[...].astype(BF)
        last(dk_ref).start()

    @pl.when(core == 1)
    def _():
        dv_ref[...] = acc[...].astype(BF)
        last(dv_ref).start()

    def close_up(j, _):
        send_a(me + 1 + j).wait_send()
        return 0

    lax.fori_loop(0, S - 1 - me, close_up, 0)

    def close_down(s, _):
        forward(mate, s).wait_send()
        swap(s).wait_send()
        give_back(s).wait_send()
        return 0

    lax.fori_loop(0, me, close_down, 0)
    own_swap.wait_send()

    @pl.when(core == 0)
    def _():
        last(dk_ref).wait_send()
        last(dv_ref).wait_recv()

    @pl.when(core == 1)
    def _():
        last(dv_ref).wait_send()
        last(dk_ref).wait_recv()


def place_kernel(*refs):
    n = len(refs) // 2
    moves = [pltpu.make_async_copy(refs[i], refs[n + i], refs[-1].at[i]) for i in range(n)]
    for move in moves:
        move.start()
    for move in moves:
        move.wait()


def place(*arrays):
    return pl.pallas_call(
        place_kernel,
        out_shape=tuple(jax.ShapeDtypeStruct(a.shape, a.dtype) for a in arrays),
        in_specs=[pl.BlockSpec(memory_space=pltpu.VMEM)] * len(arrays),
        out_specs=(pl.BlockSpec(memory_space=pl.ANY),) * len(arrays),
        scratch_shapes=[pltpu.SemaphoreType.DMA((len(arrays),))],
        compiler_params=pltpu.CompilerParams(vmem_limit_bytes=65536),
    )(*(pltpu.with_memory_space_constraint(a, pltpu.VMEM) for a in arrays))


def per_device(queries, grad_out, keys, values, indices, valid):
    tokens, _, heads, width = queries.shape
    S = lax.axis_size("seq")
    total, topk = indices.shape[1:]
    nb = tokens // BLK
    chunk = CAP * BLK
    nrem = (S - 1) * chunk
    own_rows = tokens
    nkeys = nrem + own_rows
    rows = tokens * heads
    rows_b = BLK * heads
    lanes = -(-total // 128) * 128
    slot_lanes = -(-(nkeys // BLK) // 128) * 128
    pre = S <= 4
    cfg = (S, heads, nb, total, topk, width, pre)
    vmem = pl.BlockSpec(memory_space=pltpu.VMEM)
    hbm = pl.BlockSpec(memory_space=pl.ANY)
    dma = pltpu.SemaphoreType.DMA
    dq, dk, dv = pl.pallas_call(
        functools.partial(kernel, cfg),
        out_shape=(
            pltpu.VMEM((rows, width), BF),
            pltpu.VMEM((own_rows, width), BF),
            pltpu.VMEM((own_rows, width), BF),
        ),
        in_specs=[hbm] * 6,
        out_specs=(vmem, vmem, vmem),
        scratch_shapes=[
            pltpu.VMEM((total, lanes), F32),
            pltpu.VMEM((width + slot_lanes, rows), BF),
            pltpu.VMEM((2, rows, width), BF),
            pltpu.VMEM((2, own_rows, width), BF),
            pltpu.VMEM((nkeys, slot_lanes), BF),
            pltpu.VMEM((width, nkeys), BF),
            pltpu.VMEM((S - 1, width, chunk), BF),
            pltpu.VMEM((width, own_rows), BF),
            pltpu.VMEM((width, rows), F32),
            pltpu.VMEM((width, rows), BF),
            pltpu.VMEM((S, chunk, width), BF),
            pltpu.VMEM((2, nrem, width), BF),
            pltpu.VMEM((S if pre else 1, own_rows, chunk), BF),
            pltpu.VMEM((nb, max(own_rows, chunk), rows_b), F32),
            pltpu.VMEM((2, nkeys, rows), BF),
            pltpu.VMEM((chunk, rows), BF),
            pltpu.VMEM((S, 2, chunk, width), F32),
            pltpu.VMEM((S, chunk, width), F32),
            pltpu.VMEM((S, chunk, width), BF),
            pltpu.VMEM((S, chunk, width), BF),
            pltpu.VMEM((own_rows, width), F32),
            pltpu.VMEM((own_rows, width), F32),
            pltpu.VMEM((own_rows, width), F32),
            dma((S,)), dma((S,)), dma((S,)), dma((S,)), dma((S,)), dma((S,)),
            dma((S,)), dma((S,)), dma((2,)), dma((2,)),
            dma((6,)),
            pltpu.SemaphoreType.REGULAR((S,)),
            pltpu.VMEM((2, topk, total), jnp.int32),
            pltpu.VMEM((S, nb, rows_b), F32),
            pltpu.VMEM((S, nb, rows_b), F32),
            pltpu.VMEM((S, nb, rows_b), F32),
        ],
        compiler_params=pltpu.CompilerParams(
            collective_id=0, has_side_effects=True, vmem_limit_bytes=67043328 - 6 * own_rows * width * 2 - 4096
        ),
    )(
        queries.reshape(rows, width),
        grad_out.reshape(rows, width),
        keys.reshape(own_rows, width),
        values.reshape(own_rows, width),
        indices[0].T,
        valid[0].T,
    )
    dq, dk, dv = place(dq, dk, dv)
    return (
        dq.reshape(tokens, 1, heads, width),
        dk.reshape(tokens, 1, width),
        dv.reshape(tokens, 1, width),
    )


def solution(mesh):
    return jax.shard_map(
        per_device,
        mesh=mesh,
        in_specs=(
            P(("groups", "seq"), "head", "inner", None),
            P(("groups", "seq"), "head", "inner", None),
            P(("groups", "seq"), "head", None),
            P(("groups", "seq"), "head", None),
            P("head", "groups", None),
            P("head", "groups", None),
        ),
        out_specs=(
            P(("groups", "seq"), "head", "inner", None),
            P(("groups", "seq"), "head", None),
            P(("groups", "seq"), "head", None),
        ),
        check_vma=False,
    )
```
